32 devices in a mesh: dp: 32 (over z, y, x, core).
Axes of the slice: x: 2, y: 2, z: 4, core: 2. Of those that a mesh axis runs over, the one named last changes fastest.
Arguments:
- token_ids: int32 [32768], P('dp'), may hold values from 0 to 31999, as said below
- tokens: bfloat16 [32768, 4096], P('dp'), may hold values from -64 to 64
- frozen_weight: bfloat16 [4096, 1024], replicated, may hold values from -0.09375 to 0.09375
- adapter_down: bfloat16 [4096, 128], replicated, may hold values from -0.09375 to 0.09375
- adapter_up: bfloat16 [128, 1024], replicated, may hold values from -1.5 to 1.5
- gate_weight: bfloat16 [4096, 8], replicated, may hold values from -1 to 1
- upstream: bfloat16 [32768, 1024], P('dp'), may hold values from -6 to 6
Outputs:
- projected: bfloat16 [32768, 1024], P('dp')
- input_grad: bfloat16 [32768, 4096], P('dp')
- clipped_down: float32 [4096, 128], replicated
- clipped_up: float32 [128, 1024], replicated
- clipped_gate: float32 [4096, 8], replicated
- load: float32 [8], replicated
- entropy: float32 [], replicated
The draws below stay inside these ranges and needn't reach their ends.
Inputs may be any that keep to these rules, and one draw needn't show every extreme that they name: `token_ids`: within each device's block of 1024 tokens the live tokens (id not 0) come first, 256 or more of them, and padding (id 0) fills the rest; the last block is wholly live.
All inputs are finite; a program needn't handle non-finite values.
Results may differ from the reference program's by a relative error of at most 0.0095.
Values sent between devices are 32-bit elements; how exact they have to be, the bound alone decides.
No kernel may reach another device: no remote copies, remote signals or barrier semaphores. Data moves between devices by JAX's collectives and lax.ppermute only.
A program may use at most 192 MiB of HBM per device.

```python
import math
import jax
import jax.numpy as jnp
from jax import lax

D = 4096
DOUT = 1024
EXPERTS = 8
RANK = 16
VOCAB = 32000
TOK_DEV = 1024
TOKENS = 32768


def gate_table(key):
    return jax.random.normal(jax.random.fold_in(key, 7), (D, EXPERTS), jnp.float32) * (2.0 / math.sqrt(D))


def draw_gate_weight(key, part):
    return jnp.clip(gate_table(key), -1.0, 1.0).astype(jnp.bfloat16)


def draw_tokens(key, part):
    base_key = jax.random.fold_in(key, 11)
    noise = jax.random.normal(jax.random.fold_in(base_key, 1), (TOKENS, D), jnp.float32)
    scales = jnp.exp(jax.random.uniform(jax.random.fold_in(base_key, 2), (TOKENS, 1), jnp.float32, -math.log(2.0), math.log(2.0)))
    rows = noise * scales
    return jnp.clip(rows, -64.0, 64.0).astype(jnp.bfloat16)


def draw_token_ids(key, part):
    blocks = TOKENS // TOK_DEV
    block_ids = jnp.arange(blocks, dtype=jnp.int32)
    lowest = TOK_DEV // 4
    rising = (TOK_DEV - lowest) * block_ids // max(blocks - 1, 1)
    jitter = jax.random.randint(jax.random.fold_in(key, 21), (blocks,), 0, TOK_DEV // 8 + 1, dtype=jnp.int32)
    length = jnp.clip(lowest + rising - jitter, lowest, TOK_DEV)
    length = length.at[blocks - 1].set(TOK_DEV)
    position = jnp.arange(TOK_DEV, dtype=jnp.int32)
    alive = position[None, :] < length[:, None]
    values = jax.random.randint(jax.random.fold_in(key, 22), (blocks, TOK_DEV), 1, VOCAB, dtype=jnp.int32)
    return jnp.where(alive, values, 0).reshape(TOKENS).astype(jnp.int32)


def level_of(rng, dims, shards, smallest, high):
    level = 1.0
    for axis_at, shards_of in shards:
        steps = jax.random.uniform(jax.random.fold_in(jax.random.fold_in(rng, 6), axis_at), (shards_of,), jnp.float32, smallest / len(shards), high / len(shards))
        level = level * jnp.repeat(jnp.exp(steps), dims[axis_at] // shards_of).reshape((-1,) + (1,) * (len(dims) - 1 - axis_at))
    return level


def normal_values(stream_key, extent, scale, most, cuts=(), kind=jnp.bfloat16):
    values = jax.random.normal(stream_key, extent, jnp.float32) * scale
    if len(cuts) > 0:
        values = level_of(stream_key, extent, cuts, -0.22, 0.18) * values
    return jnp.clip(values, min=-most, max=most).astype(kind)


def setup_inputs(seed: int = 0) -> dict:
    streams_of = jax.random.split(jax.random.key(seed), 8)
    token_ids = draw_token_ids(jax.random.fold_in(streams_of[7], 71), 0)
    tokens = draw_tokens(jax.random.fold_in(streams_of[7], 71), 0)
    frozen_weight = normal_values(streams_of[2], (D, DOUT), D ** -0.5, 0.09375)
    adapter_down = normal_values(streams_of[3], (D, EXPERTS * RANK), D ** -0.5, 0.09375)
    adapter_up = normal_values(streams_of[4], (EXPERTS * RANK, DOUT), RANK ** -0.5, 1.5)
    gate_weight = draw_gate_weight(jax.random.fold_in(streams_of[7], 71), 0)
    upstream = normal_values(streams_of[6], (TOKENS, DOUT), 1.0, 6.0, ((0, 32),))
    return dict(token_ids=token_ids, tokens=tokens, frozen_weight=frozen_weight, adapter_down=adapter_down, adapter_up=adapter_up, gate_weight=gate_weight, upstream=upstream)


def reference(token_ids, tokens, frozen_weight, adapter_down, adapter_up, gate_weight, upstream):
    live = (token_ids != 0).astype(jnp.float32)
    base = jnp.dot(tokens, frozen_weight, preferred_element_type=jnp.float32)
    logits = jnp.dot(tokens, gate_weight, preferred_element_type=jnp.float32)
    prob = jax.nn.softmax(logits, axis=1)
    logp = jax.nn.log_softmax(logits, axis=1)
    low = jnp.dot(tokens, adapter_down, preferred_element_type=jnp.float32).astype(jnp.bfloat16)
    spread = jnp.repeat(prob, RANK, axis=1)
    weighted = (low.astype(jnp.float32) * spread).astype(jnp.bfloat16)
    projected = (base + 2.0 * jnp.dot(weighted, adapter_up, preferred_element_type=jnp.float32)).astype(jnp.bfloat16)
    masked = upstream * live.astype(jnp.bfloat16)[:, None]
    grad_up = 2.0 * jnp.dot(weighted.T, masked, preferred_element_type=jnp.float32)
    back = jnp.dot(masked, adapter_up.T, preferred_element_type=jnp.float32)
    gate_task = 2.0 * lax.optimization_barrier(jnp.sum((low.astype(jnp.float32) * back).reshape(-1, EXPERTS, RANK), axis=2))
    low_grad = (2.0 * spread * back).astype(jnp.bfloat16)
    grad_down = jnp.dot(tokens.T, low_grad, preferred_element_type=jnp.float32)
    ent_tok = -lax.optimization_barrier(jnp.sum(prob * logp, axis=1))
    load_sum = lax.optimization_barrier(jnp.sum(live[:, None] * prob, axis=0))
    ent_sum = jnp.sum(live * ent_tok)
    live_sum = jnp.sum(live)

    def jac(v):
        return prob * (v - lax.optimization_barrier(jnp.sum(prob * v, axis=1, keepdims=True)))
    gate_z = jac(gate_task) + 50.0 * live[:, None] * prob * (logp + ent_tok[:, None])
    gate_z = gate_z + 2.0 * EXPERTS * 100.0 / live_sum * live[:, None] * jac(load_sum[None, :])
    grad_gate = jnp.dot(tokens.astype(jnp.float32).T, gate_z, precision=lax.Precision.HIGHEST)
    input_grad = jnp.dot(masked, frozen_weight.T, preferred_element_type=jnp.float32)
    input_grad = input_grad + jnp.dot(low_grad, adapter_down.T, preferred_element_type=jnp.float32)
    input_grad = input_grad + jnp.dot(gate_z, gate_weight.astype(jnp.float32).T, precision=lax.Precision.HIGHEST)
    total = jnp.sum(grad_down * grad_down) + jnp.sum(grad_up * grad_up) + jnp.sum(grad_gate * grad_gate)
    count = D * EXPERTS * RANK + EXPERTS * RANK * DOUT + D * EXPERTS
    clip = jnp.minimum(1.0, math.sqrt(count) / jnp.sqrt(total))
    return (projected, input_grad.astype(jnp.bfloat16), grad_down * clip, grad_up * clip, grad_gate * clip, load_sum / live_sum, ent_sum / live_sum)
```

```python
import functools
import math

import jax
import jax.numpy as jnp
from jax import lax
from jax.experimental import pallas as pl
from jax.experimental.pallas import tpu as pltpu
from jax.sharding import PartitionSpec as P

F32 = jnp.float32
BF16 = jnp.bfloat16
LANES = 128
TILES = 4
VMEM = pltpu.VMEM
SMEM = pltpu.SMEM
HIGH = 60 * 1024 * 1024


def nn(a, b):
    return lax.dot_general(a, b, (((1,), (0,)), ((), ())), preferred_element_type=F32)


def nt(a, b):
    return lax.dot_general(a, b, (((1,), (1,)), ((), ())), preferred_element_type=F32)


def split(x):
    upper = x.astype(BF16).astype(F32)
    return upper, x - upper


def count_live(ids_ref):
    return jnp.sum((ids_ref[...] != 0).astype(jnp.int32))


def place(word, order, depth):
    spot = 0
    for step in range(depth):
        spot = spot + (((word >> order[step]) & 1) << (depth - 1 - step))
    return spot


def spots(mine, pair, side, orders, depth):
    word = (mine ^ pair) & ((1 << depth) - 1)
    first = place(word, orders[0], depth)
    second = place(word, orders[1], depth)
    kept = jnp.where(side == 0, first, second)
    sent = jnp.where(side == 0, second, first)
    return kept, sent


def local_kernel(
    orders_a, orders_b, experts, where_ref, ids_ref, gate_ref, down_ref, up_ref, tok_hbm, ups_hbm,
    keep_a, send_a, keep_b, send_b, weighted_ref, lowgrad_ref, plain_ref, share_ref, wide_ref,
    tok, ups, left, left_t, weighted_t, grad_up, stats, tok_sem, ups_sem,
):
    rows, width = tok.shape
    ranks = down_ref.shape[1]
    rank = ranks // experts
    tile = rows // TILES
    for t in range(TILES):
        part = pl.ds(t * tile, tile)
        pltpu.make_async_copy(tok_hbm.at[part], tok.at[part], tok_sem.at[t]).start()
        pltpu.make_async_copy(ups_hbm.at[part], ups.at[part], ups_sem.at[t]).start()
    mine, side = where_ref[0], where_ref[1]
    count = count_live(ids_ref)
    row_i = lax.broadcasted_iota(jnp.int32, (experts, ranks), 0)
    col_i = lax.broadcasted_iota(jnp.int32, (experts, ranks), 1)
    repeat = (col_i // rank == row_i).astype(BF16)
    gate_t = gate_ref[...].astype(F32).T.astype(BF16)
    wide_ref[:, :ranks] = down_ref[...]
    wide_ref[:, ranks:] = nn(gate_t, repeat).astype(BF16)
    up = up_ref[...]
    r2 = lax.broadcasted_iota(jnp.int32, (2 * ranks, ranks), 0)
    c2 = lax.broadcasted_iota(jnp.int32, (2 * ranks, ranks), 1)
    group = ((r2 % ranks) // rank == c2 // rank).astype(BF16)
    r1 = lax.broadcasted_iota(jnp.int32, (ranks, ranks), 0)
    c1 = lax.broadcasted_iota(jnp.int32, (ranks, ranks), 1)
    regroup = ((r1 % rank) * experts + r1 // rank == c1).astype(BF16)
    slot = lax.broadcasted_iota(jnp.int32, (tile, ranks), 1) % rank
    load = jnp.zeros((1, ranks), F32)
    entropy = jnp.zeros((1, 1), F32)
    for t in range(TILES):
        part = pl.ds(t * tile, tile)
        pltpu.make_async_copy(tok_hbm.at[part], tok.at[part], tok_sem.at[t]).wait()
        pltpu.make_async_copy(ups_hbm.at[part], ups.at[part], ups_sem.at[t]).wait()
        live = lax.broadcasted_iota(jnp.int32, (tile, 1), 0) + t * tile < count
        alive = live.astype(F32)
        both = nn(tok[part, :], wide_ref[...])
        low = both[:, :ranks].astype(BF16).astype(F32)
        logits = both[:, ranks:]
        shifted = logits - jnp.max(logits, axis=1, keepdims=True)
        powers = jnp.exp(shifted)
        total = jnp.sum(powers, axis=1, keepdims=True) * (1.0 / rank)
        prob = powers / total
        logp = shifted - jnp.log(total)
        weighted = (low * prob).astype(BF16)
        weighted_ref[part, :] = weighted
        weighted_t[:, part] = weighted.astype(F32).T.astype(BF16)
        ent = -jnp.sum(prob * logp, axis=1, keepdims=True) * (1.0 / rank)
        masked = jnp.where(live, ups[part, :].astype(F32), 0.0).astype(BF16)
        ups[part, :] = masked
        back = nt(masked, up)
        low_grad = (2.0 * prob * back).astype(BF16)
        lowgrad_ref[part, :] = low_grad
        big, small = split(low * back)
        task = 2.0 * nn(jnp.concatenate([big, small], axis=1).astype(BF16), group)
        inner = jnp.sum(prob * task, axis=1, keepdims=True) * (1.0 / rank)
        share = alive * prob
        plain = prob * (task - inner) + 50.0 * share * (logp + ent)
        plain_ref[part, :] = plain
        share_ref[part, :] = share
        load = load + jnp.sum(share, axis=0, keepdims=True)
        entropy = entropy + jnp.sum(alive * ent, axis=0, keepdims=True)
        chosen = jnp.zeros((tile, ranks), F32)
        for step in range(experts // 2 + 1):
            value = plain if step == 0 else share * pltpu.roll(prob, ranks - rank * step, 1)
            big, small = split(value)
            chosen = jnp.where(slot == 2 * step, big, chosen)
            chosen = jnp.where(slot == 2 * step + 1, small, chosen)
        picked = nn(chosen.astype(BF16), regroup)
        left_t[:ranks, part] = low_grad.astype(F32).T.astype(BF16)
        left_t[ranks:, part] = picked.T.astype(BF16)
    grad_up[...] = 2.0 * nn(weighted_t[...], ups[...])
    stat_row = lax.broadcasted_iota(jnp.int32, (8, ranks), 0)
    stats[...] = jnp.where(
        stat_row == 0,
        load,
        jnp.where(stat_row == 1, entropy, jnp.where(stat_row == 2, count.astype(F32), 0.0)),
    )
    kinds = experts // 2 + 1
    used = ranks + 2 * kinds * experts
    pairs = width // (2 * LANES)
    depth = pairs.bit_length() - 1
    gate_rows = kinds * experts
    up_rows = ranks * up_ref.shape[1] // (2 * pairs * LANES)
    per = ranks // up_rows
    for pair in range(pairs):
        kept_a, sent_a = spots(mine, pair, side, orders_a, depth)
        kept_b, sent_b = spots(mine, pair, side, orders_b, depth)
        piece = nn(left_t[:used, :], tok[:, pl.ds(pair * 2 * LANES, 2 * LANES)])
        one, two = piece[:, :LANES], piece[:, LANES:]
        keep = jnp.where(side == 0, one, two)
        send = jnp.where(side == 0, two, one)
        keep_a[kept_a] = keep[:ranks]
        send_a[sent_a] = send[:ranks]
        for kind in range(kinds):
            at = ranks + 2 * kind * experts
            to = pl.ds(kind * experts, experts)
            keep_b[kept_b, to] = keep[at : at + experts] + keep[at + experts : at + 2 * experts]
            send_b[sent_b, to] = send[at : at + experts] + send[at + experts : at + 2 * experts]
        keep_b[kept_b, pl.ds(gate_rows, 8)] = stats[...]
        send_b[sent_b, pl.ds(gate_rows, 8)] = stats[...]
        first, second = 2 * pair, 2 * pair + 1
        one = grad_up[pl.ds((first % per) * up_rows, up_rows), pl.ds(first // per * LANES, LANES)]
        two = grad_up[pl.ds((second % per) * up_rows, up_rows), pl.ds(second // per * LANES, LANES)]
        to = pl.ds(gate_rows + 8, up_rows)
        keep_b[kept_b, to] = jnp.where(side == 0, one, two)
        send_b[sent_b, to] = jnp.where(side == 0, two, one)


def local_grads(where, ids, gate_t, down, up, tokens, upstream, orders_a, orders_b):
    rows, width = tokens.shape
    outs = upstream.shape[1]
    experts, ranks = gate_t.shape[0], down.shape[1]
    pairs = width // (2 * LANES)
    kinds = experts // 2 + 1
    rows_b = kinds * experts + 8 + ranks * outs // (2 * pairs * LANES)
    any_spec = pl.BlockSpec(memory_space=pl.ANY)
    vmem = pl.BlockSpec(memory_space=VMEM)
    return pl.pallas_call(
        functools.partial(local_kernel, orders_a, orders_b, experts),
        out_shape=[
            jax.ShapeDtypeStruct((pairs, ranks, LANES), F32),
            jax.ShapeDtypeStruct((pairs, ranks, LANES), F32),
            jax.ShapeDtypeStruct((pairs, rows_b, LANES), F32),
            jax.ShapeDtypeStruct((pairs, rows_b, LANES), F32),
            jax.ShapeDtypeStruct((rows, ranks), BF16),
            jax.ShapeDtypeStruct((rows, ranks), BF16),
            jax.ShapeDtypeStruct((rows, ranks), F32),
            jax.ShapeDtypeStruct((rows, ranks), F32),
            jax.ShapeDtypeStruct((width, 2 * ranks), BF16),
        ],
        in_specs=[pl.BlockSpec(memory_space=SMEM), vmem, vmem, vmem, vmem, any_spec, any_spec],
        out_specs=[vmem] * 9,
        scratch_shapes=[
            VMEM((rows, width), BF16),
            VMEM((rows, outs), BF16),
            VMEM((8, LANES), F32),
            VMEM((2 * ranks, rows), BF16),
            VMEM((ranks, rows), BF16),
            VMEM((ranks, outs), F32),
            VMEM((8, ranks), F32),
            pltpu.SemaphoreType.DMA((TILES,)),
            pltpu.SemaphoreType.DMA((TILES,)),
        ],
        compiler_params=pltpu.CompilerParams(vmem_limit_bytes=HIGH),
        cost_estimate=pl.CostEstimate(
            flops=2 * rows * width * 512, bytes_accessed=2 * rows * (width + outs), transcendentals=0
        ),
        name="local_grads",
    )(where, ids, gate_t, down, up, tokens, upstream)


def project_kernel(tok_ref, weighted_ref, frozen_ref, up_ref, out_ref):
    base = nn(tok_ref[...], frozen_ref[...])
    out_ref[...] = (base + 2.0 * nn(weighted_ref[...], up_ref[...])).astype(BF16)


def project(tokens, weighted, frozen, up):
    rows, width = tokens.shape
    outs, ranks = frozen.shape[1], up.shape[0]
    tile = rows // TILES
    return pl.pallas_call(
        project_kernel,
        grid=(TILES,),
        out_shape=jax.ShapeDtypeStruct((rows, outs), BF16),
        in_specs=[
            pl.BlockSpec((tile, width), lambda i: (i, 0)),
            pl.BlockSpec((tile, ranks), lambda i: (i, 0)),
            pl.BlockSpec((width, outs), lambda i: (0, 0)),
            pl.BlockSpec((ranks, outs), lambda i: (0, 0)),
        ],
        out_specs=pl.BlockSpec((tile, outs), lambda i: (i, 0)),
        compiler_params=pltpu.CompilerParams(vmem_limit_bytes=HIGH),
        cost_estimate=pl.CostEstimate(
            flops=2 * rows * outs * (width + ranks),
            bytes_accessed=2 * (rows * width + width * outs + rows * outs),
            transcendentals=0,
        ),
        name="project",
    )(tokens, weighted, frozen, up)


def owner_kernel(experts, keep_ref, recv_ref, out_ref, stats_ref):
    block = keep_ref[0] + recv_ref[0]
    kinds = experts // 2 + 1
    at = kinds * experts
    stats = block[at : at + 8]
    stats_ref[...] = stats
    rank = LANES // experts
    row = lax.broadcasted_iota(jnp.int32, (experts, LANES), 0)
    lane = lax.broadcasted_iota(jnp.int32, (experts, LANES), 1)
    weight = jnp.broadcast_to(stats[0:1], (experts, LANES))

    def column(step):
        hit = lane == (row + step) % experts * rank
        return jnp.sum(jnp.where(hit, weight, 0.0), axis=1, keepdims=True)

    mine = column(0)
    total = jnp.zeros((experts, LANES), F32)
    for step in range(1, kinds):
        both = block[step * experts : (step + 1) * experts]
        total = total + both * (mine - column(step))
        if 2 * step != experts:
            total = total + pltpu.roll(both, step, 0) * (mine - column(experts - step))
    scale = 2.0 * experts * 100.0 / stats[2:3]
    out_ref[0, :experts] = block[:experts] + scale * total
    out_ref[0, experts:] = block[at + 8 :]


def owner_rows(keep, recv, experts):
    kinds = experts // 2 + 1
    rows = keep.shape[1] - kinds * experts - 8 + experts
    return pl.pallas_call(
        functools.partial(owner_kernel, experts),
        out_shape=[
            jax.ShapeDtypeStruct((1, rows, LANES), F32),
            jax.ShapeDtypeStruct((8, LANES), F32),
        ],
        name="owner_rows",
    )(keep, recv)


def input_kernel(experts, ids_ref, ups_ref, lowgrad_ref, plain_ref, share_ref, stats_ref, frozen_ref, wide_ref, out_ref, left):
    rows, outs = ups_ref.shape
    ranks = lowgrad_ref.shape[1]
    rank = ranks // experts

    @pl.when(pl.program_id(0) == 0)
    def _():
        count = count_live(ids_ref)
        tile = rows // TILES
        weight = stats_ref[0:1, :]
        scale = 2.0 * experts * 100.0 / stats_ref[2:3, :]
        slot = lax.broadcasted_iota(jnp.int32, (tile, ranks), 1) % rank
        for t in range(TILES):
            part = pl.ds(t * tile, tile)
            live = lax.broadcasted_iota(jnp.int32, (tile, 1), 0) + t * tile < count
            left[part, :outs] = jnp.where(live, ups_ref[part, :].astype(F32), 0.0).astype(BF16)
            left[part, outs : outs + ranks] = lowgrad_ref[part, :]
            share = share_ref[part, :]
            inner = jnp.sum(share * weight, axis=1, keepdims=True) * (1.0 / rank)
            value = plain_ref[part, :] + scale * share * (weight - inner)
            big, small = split(value)
            left[part, outs + ranks :] = jnp.where(
                slot == 0, big, jnp.where(slot == 1, small, 0.0)
            ).astype(BF16)

    out_ref[...] = (
        nt(left[:, :outs], frozen_ref[...]) + nt(left[:, outs:], wide_ref[...])
    ).astype(BF16)


def input_grads(ids, upstream, low_grad, plain, share, stats, frozen, wide, experts):
    rows, outs = upstream.shape
    width, ranks = frozen.shape[0], low_grad.shape[1]
    steps = 8
    tile = width // steps
    whole = lambda i: (0, 0)
    return pl.pallas_call(
        functools.partial(input_kernel, experts),
        grid=(steps,),
        out_shape=jax.ShapeDtypeStruct((rows, width), BF16),
        in_specs=[
            pl.BlockSpec(ids.shape, whole),
            pl.BlockSpec((rows, outs), whole),
            pl.BlockSpec((rows, ranks), whole),
            pl.BlockSpec((rows, ranks), whole),
            pl.BlockSpec((rows, ranks), whole),
            pl.BlockSpec(stats.shape, whole),
            pl.BlockSpec((tile, outs), lambda i: (i, 0)),
            pl.BlockSpec((tile, 2 * ranks), lambda i: (i, 0)),
        ],
        out_specs=pl.BlockSpec((rows, tile), lambda i: (0, i)),
        scratch_shapes=[VMEM((rows, outs + 2 * ranks), BF16)],
        compiler_params=pltpu.CompilerParams(vmem_limit_bytes=HIGH),
        cost_estimate=pl.CostEstimate(
            flops=2 * rows * width * (outs + 2 * ranks),
            bytes_accessed=2 * (rows * width + width * outs + rows * outs),
            transcendentals=0,
        ),
        name="input_grads",
    )(ids, upstream, low_grad, plain, share, stats, frozen, wide)


def clip_kernel(orders_a, orders_b, experts, limit, where_ref, own_a, other_a, own_b, other_b, stat_own, stat_other, down_ref, up_ref, gate_ref, load_ref):
    mine, side = where_ref[0], where_ref[1]
    pairs, ranks = own_a.shape[0], own_a.shape[1]
    depth = pairs.bit_length() - 1
    up_rows = own_b.shape[1] - experts
    per = ranks // up_rows

    def fold(block):
        square = block * block
        return jnp.sum(square.reshape(block.shape[0] // 8, 8, LANES), axis=0)

    def measure(pair, sums):
        kept_a, sent_a = spots(mine, pair, side, orders_a, depth)
        kept_b, sent_b = spots(mine, pair, side, orders_b, depth)
        first = sums[0] + fold(own_a[kept_a]) + fold(own_b[kept_b])
        second = sums[1] + fold(other_a[sent_a]) + fold(other_b[sent_b])
        return first, second

    zero = jnp.zeros((8, LANES), F32)
    sums = lax.fori_loop(0, pairs, measure, (zero, zero))
    total = jnp.sum(sums[0] + sums[1], axis=(0, 1), keepdims=True)
    factor = jnp.minimum(1.0, limit / jnp.sqrt(total))

    def emit(block_a, block_b, at):
        down_ref[pl.ds(pl.multiple_of(at * LANES, LANES), LANES), :] = (block_a * factor).T
        lanes = pl.ds(pl.multiple_of(at * LANES, LANES), LANES)
        gate_ref[:, lanes] = block_b[:experts] * factor
        rows = pl.ds(pl.multiple_of(at % per * up_rows, up_rows), up_rows)
        lanes = pl.ds(pl.multiple_of(at // per * LANES, LANES), LANES)
        up_ref[rows, lanes] = block_b[experts:] * factor

    def write(pair, carry):
        kept_a, sent_a = spots(mine, pair, side, orders_a, depth)
        kept_b, sent_b = spots(mine, pair, side, orders_b, depth)
        emit(own_a[kept_a], own_b[kept_b], 2 * pair + side)
        emit(other_a[sent_a], other_b[sent_b], 2 * pair + 1 - side)
        return carry

    lax.fori_loop(0, pairs, write, 0)
    stats = jnp.where(side == 0, stat_own[...], stat_other[...])
    load_ref[...] = stats / stats[2:3]


def clip_write(where, own_a, other_a, own_b, other_b, stat_own, stat_other, outs, experts, orders_a, orders_b):
    pairs, ranks = own_a.shape[0], own_a.shape[1]
    width = 2 * pairs * LANES
    limit = math.sqrt(width * ranks + ranks * outs + width * experts)
    vmem = pl.BlockSpec(memory_space=VMEM)
    return pl.pallas_call(
        functools.partial(clip_kernel, orders_a, orders_b, experts, limit),
        out_shape=[
            jax.ShapeDtypeStruct((width, ranks), F32),
            jax.ShapeDtypeStruct((ranks, outs), F32),
            jax.ShapeDtypeStruct((experts, width), F32),
            jax.ShapeDtypeStruct((8, LANES), F32),
        ],
        in_specs=[pl.BlockSpec(memory_space=SMEM)] + [vmem] * 6,
        out_specs=[vmem] * 4,
        compiler_params=pltpu.CompilerParams(vmem_limit_bytes=HIGH),
        name="clip_write",
    )(where, own_a, other_a, own_b, other_b, stat_own, stat_other)


def swap(array, masks):
    size = lax.axis_size("dp")
    return lax.ppermute(array, "dp", [(i, i ^ masks[i & 1]) for i in range(size)])


def halve(keep, recv):
    half = keep.shape[0] // 2
    send = keep[half:] + recv[half:]
    return keep[:half] + recv[:half], send


def on_device(token_ids, tokens, frozen, down, up, gate, upstream):
    experts = gate.shape[1]
    rank = down.shape[1] // experts
    outs = frozen.shape[1]
    rows = tokens.shape[0]
    size = lax.axis_size("dp")
    bits = size.bit_length() - 2
    depth = (tokens.shape[1] // (2 * LANES)).bit_length() - 1
    rest = tuple(range(2, bits))
    orders_a = ((0, 1) + rest, (1, 0) + rest)
    orders_b = ((0, 1) + rest, (1, 0) + rest)
    me = lax.axis_index("dp")
    where = jnp.stack([me >> 1, me & 1]).astype(jnp.int32)
    ids = token_ids.reshape(rows // LANES, LANES)
    masks_a = [(2 << orders_a[0][s], 2 << orders_a[1][s]) for s in range(bits)]
    masks_b = [(2 << orders_b[0][s], 2 << orders_b[1][s]) for s in range(bits)]

    keep_a, send_a, keep_b, send_b, weighted, low_grad, plain, share, wide = local_grads(
        where, ids, gate.T, down, up, tokens, upstream, orders_a, orders_b
    )
    recv_b = swap(send_b, (1, 1))
    recv_a = swap(send_a, (1, 1))
    projected = project(tokens, weighted, frozen, up)
    for step in range(bits):
        if step < depth:
            keep_b, send_b = halve(keep_b, recv_b)
            keep_a, send_a = halve(keep_a, recv_a)
        else:
            keep_b = send_b = keep_b + recv_b
            keep_a = send_a = keep_a + recv_a
        recv_b = swap(send_b, masks_b[step])
        recv_a = swap(send_a, masks_a[step])
    own_b, stats = owner_rows(keep_b, recv_b, experts)
    own_a = keep_a + recv_a
    input_grad = input_grads(ids, upstream, low_grad, plain, share, stats, frozen, wide, experts)
    stat_other = swap(stats, (1, 1))
    for step in reversed(range(depth)):
        own_b = jnp.concatenate([own_b, swap(own_b, masks_b[step])], axis=0)
        own_a = jnp.concatenate([own_a, swap(own_a, masks_a[step])], axis=0)
    other_b = swap(own_b, (1, 1))
    other_a = swap(own_a, (1, 1))
    clipped_down, clipped_up, clipped_gate, summary = clip_write(
        where, own_a, other_a, own_b, other_b, stats, stat_other, outs, experts, orders_a, orders_b
    )
    return (
        projected,
        input_grad,
        clipped_down,
        clipped_up,
        clipped_gate.T,
        summary[0, ::rank],
        summary[1, 0],
    )


def solution(mesh):
    placed = (P("dp"), P("dp", None), P(), P(), P(), P(), P("dp", None))
    return jax.shard_map(
        on_device,
        mesh=mesh,
        in_specs=placed,
        out_specs=(P("dp", None), P("dp", None), P(), P(), P(), P(), P()),
        check_vma=False,
    )
```

```python
import functools
import math

import jax
import jax.numpy as jnp
from jax import lax
from jax.experimental import pallas as pl
from jax.experimental.pallas import tpu as pltpu
from jax.sharding import PartitionSpec as P

F32 = jnp.float32
BF16 = jnp.bfloat16
LANES = 128
TILES = 4
VMEM = pltpu.VMEM
SMEM = pltpu.SMEM
HBM = pltpu.HBM
MIB = 1024 * 1024


def nn(a, b):
    return lax.dot_general(a, b, (((1,), (0,)), ((), ())), preferred_element_type=F32)


def nt(a, b):
    return lax.dot_general(a, b, (((1,), (1,)), ((), ())), preferred_element_type=F32)


def split(x):
    upper = x.astype(BF16).astype(F32)
    return upper, x - upper


def place(word, order, depth):
    spot = 0
    for step in range(depth):
        spot = spot + (((word >> order[step]) & 1) << (depth - 1 - step))
    return spot


def spots(mine, pair, side, orders, depth):
    word = (mine ^ pair) & ((1 << depth) - 1)
    first = place(word, orders[0], depth)
    second = place(word, orders[1], depth)
    kept = jnp.where(side == 0, first, second)
    sent = jnp.where(side == 0, second, first)
    return kept, sent


def local_kernel(
    orders_a, orders_b, where_ref, ids_hbm, gate_hbm, down_hbm, up_hbm, tok_hbm, ups_hbm, frozen_hbm,
    keep_a, send_a, keep_b, send_b, weighted_ref, lowgrad_ref, plain_ref, share_ref, wide_ref, ups,
    tok, up, frozen, ids, gate, down, both, back, left_t, weighted_t, grad_up, stats, sem, tok_sem, ups_sem,
):
    rows, width = tok.shape
    experts, ranks = gate.shape[0], down.shape[1]
    rank = ranks // experts
    tile = rows // TILES

    def fetch(source, target, flag):
        return pltpu.make_async_copy(source, target, flag)

    def tok_copy(t):
        part = pl.ds(t * tile, tile)
        return fetch(tok_hbm.at[part], tok.at[part], tok_sem.at[t])

    def ups_copy(t):
        part = pl.ds(t * tile, tile)
        return fetch(ups_hbm.at[part], ups.at[part], ups_sem.at[t])

    gate_copy = fetch(gate_hbm, gate, sem.at[0])
    down_copy = fetch(down_hbm, down, sem.at[1])
    ids_copy = fetch(ids_hbm, ids, sem.at[2])
    up_copy = fetch(up_hbm, up, sem.at[3])
    gate_copy.start()
    down_copy.start()
    ids_copy.start()
    up_copy.start()
    for t in range(TILES):
        tok_copy(t).start()
        ups_copy(t).start()
    frozen_copy = fetch(frozen_hbm, frozen, sem.at[4])
    frozen_copy.start()
    mine, side = where_ref[0], where_ref[1]
    row_i = lax.broadcasted_iota(jnp.int32, (experts, ranks), 0)
    col_i = lax.broadcasted_iota(jnp.int32, (experts, ranks), 1)
    twice = ((col_i % experts == row_i) & (col_i < 2 * experts)).astype(BF16)
    gate_copy.wait()
    wide_ref[:, ranks:] = nn(gate[...].astype(F32).T.astype(BF16), twice).astype(BF16)
    down_copy.wait()
    wide_ref[:, :ranks] = down[...]
    ids_copy.wait()
    count = jnp.sum((ids[...] != 0).astype(jnp.int32))
    up_copy.wait()
    for t in range(TILES):
        part = pl.ds(t * tile, tile)
        tok_copy(t).wait()
        both[part, :] = nn(tok[part, :], wide_ref[...])
        ups_copy(t).wait()
        live = lax.broadcasted_iota(jnp.int32, (tile, 1), 0) + t * tile < count
        ups[part, :] = ups[part, :] * live.astype(F32).astype(BF16)
        back[part, :] = nt(ups[part, :], up[...])
    logits = both[:, ranks:].T[:experts, :]
    shifted = logits - jnp.max(logits, axis=0, keepdims=True)
    powers = jnp.exp(shifted)
    total = jnp.sum(powers, axis=0, keepdims=True)
    prob = powers / total
    logp = shifted - jnp.log(total)
    ent = -jnp.sum(prob * logp, axis=0, keepdims=True)
    alive = (lax.broadcasted_iota(jnp.int32, (1, rows), 1) < count).astype(F32)
    share = alive * prob
    share_ref[...] = share
    big, rest = split(prob)
    mid, small = split(rest)
    parts = jnp.concatenate([big, mid, small], axis=0).T.astype(BF16)
    row_p = lax.broadcasted_iota(jnp.int32, (3 * experts, ranks), 0)
    col_p = lax.broadcasted_iota(jnp.int32, (3 * experts, ranks), 1)
    spread_by = (row_p % experts == col_p // rank).astype(BF16)
    row_g = lax.broadcasted_iota(jnp.int32, (experts, 2 * ranks), 0)
    col_g = lax.broadcasted_iota(jnp.int32, (experts, 2 * ranks), 1)
    group = ((col_g % ranks) // rank == row_g).astype(BF16)
    tasks = []
    for t in range(TILES):
        part = pl.ds(t * tile, tile)
        spread = nn(parts[t * tile : (t + 1) * tile], spread_by)
        low = both[part, :ranks].astype(BF16).astype(F32)
        weighted = (low * spread).astype(BF16)
        weighted_ref[part, :] = weighted
        weighted_t[:, part] = weighted.astype(F32).T.astype(BF16)
        low_grad = (2.0 * spread * back[part, :]).astype(BF16)
        lowgrad_ref[part, :] = low_grad
        left_t[:ranks, part] = low_grad.astype(F32).T.astype(BF16)
        big, small = split(low * back[part, :])
        tasks.append(nt(group, jnp.concatenate([big, small], axis=1).astype(BF16)))
    grad_up[...] = 2.0 * nn(weighted_t[...], ups[...])
    task = 2.0 * jnp.concatenate(tasks, axis=1)
    inner = jnp.sum(prob * task, axis=0, keepdims=True)
    plain = prob * (task - inner) + 50.0 * share * (logp + ent)
    plain_ref[...] = plain
    kinds = experts // 2 + 1
    for kind in range(kinds):
        value = plain if kind == 0 else share * pltpu.roll(prob, experts - kind, 0)
        big, small = split(value)
        at = pl.ds(ranks + 2 * kind * experts, 2 * experts)
        left_t[at, :] = jnp.concatenate([big, small], axis=0).astype(BF16)
    load = jnp.sum(share, axis=1, keepdims=True)
    entropy = jnp.sum(alive * ent, axis=1, keepdims=True)
    lane = lax.broadcasted_iota(jnp.int32, (experts, LANES), 1)
    stats[...] = jnp.where(
        lane < LANES // 2, load, jnp.where(lane < LANES // 4 * 3, entropy, count.astype(F32))
    )
    used = ranks + 2 * kinds * experts
    pairs = width // (2 * LANES)
    depth = pairs.bit_length() - 1
    gate_rows = kinds * experts
    up_rows = ranks * up.shape[1] // (2 * pairs * LANES)
    per = ranks // up_rows
    for pair in range(pairs):
        kept_a, sent_a = spots(mine, pair, side, orders_a, depth)
        kept_b, sent_b = spots(mine, pair, side, orders_b, depth)
        piece = nn(left_t[:used, :], tok[:, pl.ds(pair * 2 * LANES, 2 * LANES)])
        one, two = piece[:, :LANES], piece[:, LANES:]
        gates = []
        for kind in range(kinds):
            at = ranks + 2 * kind * experts
            gates.append(piece[at : at + experts] + piece[at + experts : at + 2 * experts])
        gates = jnp.concatenate(gates, axis=0)
        keep_a[kept_a] = jnp.where(side == 0, one[:ranks], two[:ranks])
        send_a[sent_a] = jnp.where(side == 0, two[:ranks], one[:ranks])
        to = pl.ds(0, gate_rows)
        keep_b[kept_b, to] = jnp.where(side == 0, gates[:, :LANES], gates[:, LANES:])
        send_b[sent_b, to] = jnp.where(side == 0, gates[:, LANES:], gates[:, :LANES])
        keep_b[kept_b, pl.ds(gate_rows, experts)] = stats[...]
        send_b[sent_b, pl.ds(gate_rows, experts)] = stats[...]
        first, second = 2 * pair, 2 * pair + 1
        one = grad_up[pl.ds((first % per) * up_rows, up_rows), pl.ds(first // per * LANES, LANES)]
        two = grad_up[pl.ds((second % per) * up_rows, up_rows), pl.ds(second // per * LANES, LANES)]
        to = pl.ds(gate_rows + experts, up_rows)
        keep_b[kept_b, to] = jnp.where(side == 0, one, two)
        send_b[sent_b, to] = jnp.where(side == 0, two, one)
    frozen_copy.wait()


def in_vmem(*arrays):
    return [pltpu.with_memory_space_constraint(array, VMEM) for array in arrays]


def in_hbm(*arrays):
    return [pltpu.with_memory_space_constraint(array, HBM) for array in arrays]


def local_grads(where, ids, gate_t, down, up, tokens, upstream, frozen, orders_a, orders_b):
    rows, width = tokens.shape
    outs = upstream.shape[1]
    experts, ranks = gate_t.shape[0], down.shape[1]
    pairs = width // (2 * LANES)
    kinds = experts // 2 + 1
    rows_b = (kinds + 1) * experts + ranks * outs // (2 * pairs * LANES)
    return pl.pallas_call(
        functools.partial(local_kernel, orders_a, orders_b),
        out_shape=[
            VMEM((pairs, ranks, LANES), F32),
            VMEM((pairs, ranks, LANES), F32),
            VMEM((pairs, rows_b, LANES), F32),
            VMEM((pairs, rows_b, LANES), F32),
            VMEM((rows, ranks), BF16),
            VMEM((rows, ranks), BF16),
            VMEM((experts, rows), F32),
            VMEM((experts, rows), F32),
            VMEM((width, 2 * ranks), BF16),
            VMEM((rows, outs), BF16),
            VMEM((rows, width), BF16),
            VMEM((ranks, outs), BF16),
            VMEM((width, outs), BF16),
        ],
        in_specs=[pl.BlockSpec(memory_space=SMEM)] + [pl.BlockSpec(memory_space=HBM)] * 7,
        out_specs=[pl.BlockSpec(memory_space=VMEM)] * 13,
        scratch_shapes=[
            VMEM(ids.shape, jnp.int32),
            VMEM((experts, width), BF16),
            VMEM((width, ranks), BF16),
            VMEM((rows, 2 * ranks), F32),
            VMEM((rows, ranks), F32),
            VMEM((2 * ranks, rows), BF16),
            VMEM((ranks, rows), BF16),
            VMEM((ranks, outs), F32),
            VMEM((experts, LANES), F32),
            pltpu.SemaphoreType.DMA((5,)),
            pltpu.SemaphoreType.DMA((TILES,)),
            pltpu.SemaphoreType.DMA((TILES,)),
        ],
        compiler_params=pltpu.CompilerParams(vmem_limit_bytes=20 * MIB),
        cost_estimate=pl.CostEstimate(
            flops=2 * rows * width * 512, bytes_accessed=2 * rows * (width + outs), transcendentals=0
        ),
        name="local_grads",
    )(where, *in_hbm(ids, gate_t, down, up, tokens, upstream, frozen))


def project_kernel(begin, tok, weighted_ref, frozen, up_ref, *rest):
    out_ref, out, out_sem = rest[-3:]
    parts, _, cols = out.shape

    def out_copy(c):
        target = out_ref.at[:, pl.ds((begin + c) * cols, cols)]
        return pltpu.make_async_copy(out.at[c], target, out_sem.at[c])

    for c in range(parts):
        lanes = pl.ds((begin + c) * cols, cols)
        base = nn(tok[...], frozen[:, lanes])
        out[c] = (base + 2.0 * nn(weighted_ref[...], up_ref[:, lanes])).astype(BF16)
        out_copy(c).start()
    for c in range(parts):
        out_copy(c).wait()


def project(tokens, weighted, frozen, up, begin, parts, past):
    rows, width = tokens.shape
    outs, ranks = frozen.shape[1], up.shape[0]
    cols = outs // TILES
    hbm = pl.BlockSpec(memory_space=HBM)
    vmem = pl.BlockSpec(memory_space=VMEM)
    return pl.pallas_call(
        functools.partial(project_kernel, begin),
        out_shape=HBM((rows, outs), BF16),
        in_specs=[vmem] * 4 + [hbm] * len(past),
        out_specs=hbm,
        input_output_aliases={4: 0} if past else {},
        scratch_shapes=[
            VMEM((parts, rows, cols), BF16),
            pltpu.SemaphoreType.DMA((parts,)),
        ],
        compiler_params=pltpu.CompilerParams(vmem_limit_bytes=8 * MIB),
        cost_estimate=pl.CostEstimate(
            flops=2 * rows * cols * parts * (width + ranks),
            bytes_accessed=2 * (rows * width + width * cols * parts + rows * cols * parts),
            transcendentals=0,
        ),
        name="project",
    )(*in_vmem(tokens, weighted, frozen, up), *in_hbm(*past))


def owner_kernel(experts, keep_a, keep_b, recv, own_ref, stats_ref):
    ranks = keep_a.shape[1]
    own_ref[0, :ranks] = keep_a[0] + recv[0, :ranks]
    block = keep_b[0] + recv[0, ranks:]
    kinds = experts // 2 + 1
    at = kinds * experts
    stats = block[at : at + experts]
    stats_ref[...] = stats
    mine = jnp.broadcast_to(stats[:, :1], (experts, LANES))
    total = jnp.zeros((experts, LANES), F32)
    for step in range(1, kinds):
        both = block[step * experts : (step + 1) * experts]
        total = total + both * (mine - pltpu.roll(mine, experts - step, 0))
        if 2 * step != experts:
            total = total + pltpu.roll(both, step, 0) * (mine - pltpu.roll(mine, step, 0))
    scale = 2.0 * experts * 100.0 / stats[:, LANES - 1 :]
    own_ref[0, ranks : ranks + experts] = block[:experts] + scale * total
    own_ref[0, ranks + experts :] = block[at + experts :]


def owner_rows(keep_a, keep_b, recv, experts):
    kinds = experts // 2 + 1
    rows = recv.shape[1] - kinds * experts
    return pl.pallas_call(
        functools.partial(owner_kernel, experts),
        out_shape=[
            jax.ShapeDtypeStruct((1, rows, LANES), F32),
            jax.ShapeDtypeStruct((experts, LANES), F32),
        ],
        compiler_params=pltpu.CompilerParams(vmem_limit_bytes=2 * MIB),
        name="owner_rows",
    )(keep_a, keep_b, recv)


def input_kernel(experts, begin, first, *refs):
    if first:
        masked, lowgrad_ref, plain_ref, share_ref, stats_ref, frozen, wide_ref = refs[:7]
        out_ref, left = refs[7:9]
    else:
        masked, left, frozen, wide_ref = refs[:4]
        out_ref = refs[5]
    out, out_sem = refs[-2:]
    parts, _, cols = out.shape

    def out_copy(c):
        target = out_ref.at[:, pl.ds((begin + c) * cols, cols)]
        return pltpu.make_async_copy(out.at[c], target, out_sem.at[c])

    if first:
        rows, ranks = lowgrad_ref.shape
        weight = stats_ref[:, :1]
        scale = 2.0 * experts * 100.0 / stats_ref[:, LANES - 1 :]
        share = share_ref[...]
        inner = jnp.sum(share * weight, axis=0, keepdims=True)
        value = plain_ref[...] + scale * share * (weight - inner)
        big, small = split(value)
        filler = jnp.zeros((ranks - 2 * experts, rows), F32)
        left[:, :ranks] = lowgrad_ref[...]
        left[:, ranks:] = jnp.concatenate([big, small, filler], axis=0).T.astype(BF16)
    for c in range(parts):
        part = pl.ds((begin + c) * cols, cols)
        out[c] = (nt(masked[...], frozen[part, :]) + nt(left[...], wide_ref[part, :])).astype(BF16)
        out_copy(c).start()
    for c in range(parts):
        out_copy(c).wait()


def input_grads(masked, lefts, frozen, wide, experts, begin, parts, past):
    rows, outs = masked.shape
    width, ranks = frozen.shape[0], wide.shape[1] // 2
    cols = 4 * LANES
    first = not past
    hbm = pl.BlockSpec(memory_space=HBM)
    vmem = pl.BlockSpec(memory_space=VMEM)
    out = HBM((rows, width), BF16)
    return pl.pallas_call(
        functools.partial(input_kernel, experts, begin, first),
        out_shape=[out, VMEM((rows, 2 * ranks), BF16)] if first else out,
        in_specs=[vmem] * (3 + len(lefts)) + [hbm] * len(past),
        out_specs=[hbm, vmem] if first else hbm,
        input_output_aliases={} if first else {4: 0},
        scratch_shapes=[
            VMEM((parts, rows, cols), BF16),
            pltpu.SemaphoreType.DMA((parts,)),
        ],
        compiler_params=pltpu.CompilerParams(vmem_limit_bytes=14 * MIB),
        cost_estimate=pl.CostEstimate(
            flops=2 * rows * cols * parts * (outs + 2 * ranks),
            bytes_accessed=2 * (rows + outs) * cols * parts + 2 * rows * outs,
            transcendentals=0,
        ),
        name="input_grads",
    )(*in_vmem(masked, *lefts, frozen, wide), *in_hbm(*past))


def clip_kernel(orders_a, orders_b, experts, limit, where_ref, own_a, other_a, own_b, other_b, stat_own, stat_other, down_ref, up_ref, gate_ref, load_ref):
    mine, side = where_ref[0], where_ref[1]
    pairs, ranks = own_a.shape[0], own_a.shape[1]
    depth = pairs.bit_length() - 1
    up_rows = own_b.shape[1] - experts
    per = ranks // up_rows

    def fold(block):
        square = block * block
        return jnp.sum(square.reshape(block.shape[0] // 8, 8, LANES), axis=0)

    def measure(pair, sums):
        kept_a, sent_a = spots(mine, pair, side, orders_a, depth)
        kept_b, sent_b = spots(mine, pair, side, orders_b, depth)
        first = sums[0] + fold(own_a[kept_a]) + fold(own_b[kept_b])
        second = sums[1] + fold(other_a[sent_a]) + fold(other_b[sent_b])
        return first, second

    zero = jnp.zeros((8, LANES), F32)
    sums = lax.fori_loop(0, pairs, measure, (zero, zero), unroll=4)
    total = jnp.sum(sums[0] + sums[1], axis=(0, 1), keepdims=True)
    factor = jnp.minimum(1.0, limit / jnp.sqrt(total))

    def emit(block_a, block_b, at):
        down_ref[pl.ds(pl.multiple_of(at * LANES, LANES), LANES), :] = (block_a * factor).T
        lanes = pl.ds(pl.multiple_of(at * LANES, LANES), LANES)
        gate_ref[:, lanes] = block_b[:experts] * factor
        rows = pl.ds(pl.multiple_of(at % per * up_rows, up_rows), up_rows)
        lanes = pl.ds(pl.multiple_of(at // per * LANES, LANES), LANES)
        up_ref[rows, lanes] = block_b[experts:] * factor

    def write(pair, carry):
        kept_a, sent_a = spots(mine, pair, side, orders_a, depth)
        kept_b, sent_b = spots(mine, pair, side, orders_b, depth)
        emit(own_a[kept_a], own_b[kept_b], 2 * pair + side)
        emit(other_a[sent_a], other_b[sent_b], 2 * pair + 1 - side)
        return carry

    lax.fori_loop(0, pairs, write, 0, unroll=4)
    stats = jnp.where(side == 0, stat_own[...], stat_other[...])
    stats = stats / stats[:, LANES - 1 :]
    row = lax.broadcasted_iota(jnp.int32, stats.shape, 0)
    lane = lax.broadcasted_iota(jnp.int32, stats.shape, 1)
    load = jnp.sum(jnp.where(row == lane, stats, 0.0), axis=0, keepdims=True)
    load_ref[...] = jnp.where(lane < LANES // 2, load, stats)


def clip_write(where, own_a, other_a, own_b, other_b, stat_own, stat_other, outs, experts, orders_a, orders_b):
    pairs, ranks = own_a.shape[0], own_a.shape[1]
    width = 2 * pairs * LANES
    limit = math.sqrt(width * ranks + ranks * outs + width * experts)
    vmem = pl.BlockSpec(memory_space=VMEM)
    return pl.pallas_call(
        functools.partial(clip_kernel, orders_a, orders_b, experts, limit),
        out_shape=[
            jax.ShapeDtypeStruct((width, ranks), F32),
            jax.ShapeDtypeStruct((ranks, outs), F32),
            jax.ShapeDtypeStruct((experts, width), F32),
            jax.ShapeDtypeStruct((experts, LANES), F32),
        ],
        in_specs=[pl.BlockSpec(memory_space=SMEM)] + [vmem] * 6,
        out_specs=[vmem] * 4,
        compiler_params=pltpu.CompilerParams(vmem_limit_bytes=24 * MIB),
        name="clip_write",
    )(where, own_a, other_a, own_b, other_b, stat_own, stat_other)


def swap(array, masks):
    size = lax.axis_size("dp")
    return lax.ppermute(array, "dp", [(i, i ^ masks[i & 1]) for i in range(size)])


def halve(keep, recv):
    half = keep.shape[0] // 2
    send = keep[half:] + recv[half:]
    return keep[:half] + recv[:half], send


def on_device(token_ids, tokens, frozen, down, up, gate, upstream):
    experts = gate.shape[1]
    outs = frozen.shape[1]
    rows = tokens.shape[0]
    size = lax.axis_size("dp")
    bits = size.bit_length() - 2
    depth = (tokens.shape[1] // (2 * LANES)).bit_length() - 1
    rest = tuple(range(2, bits))
    orders_a = ((0, 1) + rest, (1, 0) + rest)
    orders_b = ((2, 0, 1) + rest[1:], (2, 1, 0) + rest[1:])
    me = lax.axis_index("dp")
    where = jnp.stack([me >> 1, me & 1]).astype(jnp.int32)
    ids = token_ids.reshape(rows // LANES, LANES)
    masks_a = [(2 << orders_a[0][s], 2 << orders_a[1][s]) for s in range(bits)]
    masks_b = [(2 << orders_b[0][s], 2 << orders_b[1][s]) for s in range(bits)]

    keep_a, send_a, keep_b, send_b, weighted, low_grad, plain, share, wide, masked, tok, up_v, near = (
        local_grads(where, ids, gate.T, down, up, tokens, upstream, frozen, orders_a, orders_b)
    )
    split_at = keep_a.shape[1]
    recv_b = swap(send_b, (1, 1))
    recv_a = swap(send_a, (1, 1))
    filled = ()
    for step in range(bits):
        if step < depth:
            keep_b, send_b = halve(keep_b, recv_b)
            keep_a, send_a = halve(keep_a, recv_a)
        else:
            keep_b = send_b = keep_b + recv_b
            keep_a = send_a = keep_a + recv_a
        if step < 2:
            weighted, send_a, send_b, filled = lax.optimization_barrier(
                (weighted, send_a, send_b, filled)
            )
            filled = (project(tok, weighted, near, up_v, 2 * step, 2, filled),)
        if masks_a[step] == masks_b[step]:
            recv = swap(jnp.concatenate([send_a, send_b], axis=1), masks_a[step])
            recv_a, recv_b = recv[:, :split_at], recv[:, split_at:]
        else:
            recv_b = swap(send_b, masks_b[step])
            recv_a = swap(send_a, masks_a[step])
        if step < 2:
            recv_a, recv_b, filled = lax.optimization_barrier((recv_a, recv_b, filled))
    projected = filled[0]
    own, stats = owner_rows(keep_a, keep_b, recv, experts)
    own_a, own_b = own[:, :split_at], own[:, split_at:]
    lefts = (low_grad, plain, share, stats)
    filled = ()
    turns = tuple(reversed(range(depth)))
    chunk = tokens.shape[1] // (4 * LANES * depth)
    for turn, step in enumerate(turns):
        together = turn == 0 and masks_a[step] == masks_b[step]
        if together:
            lefts, own, filled = lax.optimization_barrier((lefts, own, filled))
        else:
            lefts, own_a, own_b, filled = lax.optimization_barrier((lefts, own_a, own_b, filled))
        made = input_grads(masked, lefts, near, wide, experts, turn * chunk, chunk, filled)
        if turn == 0:
            filled, lefts = (made[0],), (made[1],)
        else:
            filled = (made,)
        if together:
            recv = swap(own, masks_a[step])
            recv, filled = lax.optimization_barrier((recv, filled))
            recv_a, recv_b = recv[:, :split_at], recv[:, split_at:]
        else:
            recv_b = swap(own_b, masks_b[step])
            recv_a = swap(own_a, masks_a[step])
            recv_a, recv_b, filled = lax.optimization_barrier((recv_a, recv_b, filled))
        own_b = jnp.concatenate([own_b, recv_b], axis=0)
        own_a = jnp.concatenate([own_a, recv_a], axis=0)
    input_grad = filled[0]
    stat_other = swap(stats, (1, 1))
    other_b = swap(own_b, (1, 1))
    other_a = swap(own_a, (1, 1))
    clipped_down, clipped_up, clipped_gate, summary = clip_write(
        where, own_a, other_a, own_b, other_b, stats, stat_other, outs, experts, orders_a, orders_b
    )
    return (
        projected,
        input_grad,
        clipped_down,
        clipped_up,
        clipped_gate.T,
        summary[0, :experts],
        summary[0, LANES // 2],
    )


def solution(mesh):
    placed = (P("dp"), P("dp", None), P(), P(), P(), P(), P("dp", None))
    return jax.shard_map(
        on_device,
        mesh=mesh,
        in_specs=placed,
        out_specs=(P("dp", None), P("dp", None), P(), P(), P(), P(), P()),
        check_vma=False,
    )
```

```python
import functools
import math

import jax
import jax.numpy as jnp
from jax import lax
from jax.experimental import pallas as pl
from jax.experimental.pallas import tpu as pltpu
from jax.sharding import PartitionSpec as P


F32 = jnp.float32
BF16 = jnp.bfloat16
LANES = 128
TILES = 4
AHEAD = (1, 1, 1, 1)
CHUNKS = (0, 1, 2)
VMEM = pltpu.VMEM
SMEM = pltpu.SMEM
HBM = pltpu.HBM
MIB = 1024 * 1024


def nn(a, b):
    return lax.dot_general(a, b, (((1,), (0,)), ((), ())), preferred_element_type=F32)


def nt(a, b):
    return lax.dot_general(a, b, (((1,), (1,)), ((), ())), preferred_element_type=F32)


def split(x):
    upper = x.astype(BF16).astype(F32)
    return upper, x - upper


def place(word, order, depth):
    spot = 0
    for step in range(depth):
        spot = spot + (((word >> order[step]) & 1) << (depth - 1 - step))
    return spot


def spots(mine, pair, side, orders, depth):
    word = (mine ^ pair) & ((1 << depth) - 1)
    first = place(word, orders[0], depth)
    second = place(word, orders[1], depth)
    kept = jnp.where(side == 0, first, second)
    sent = jnp.where(side == 0, second, first)
    return kept, sent


def local_kernel(
    orders_a, orders_b, where_ref, ids_hbm, gate_hbm, down_hbm, up_hbm, tok_hbm, ups_hbm, frozen_hbm,
    keep_a, send_a, keep_b, send_b, weighted_ref, lowgrad_ref, plain_ref, share_ref, wide_ref, ups,
    tok, up, frozen, ids, gate, down, both, back, left_t, weighted_t, grad_up, stats, sem, tok_sem, ups_sem,
):
    rows, width = tok.shape
    experts, ranks = gate.shape[0], down.shape[1]
    rank = ranks // experts
    tile = rows // TILES

    def fetch(source, target, flag):
        return pltpu.make_async_copy(source, target, flag)

    def tok_copy(t):
        part = pl.ds(t * tile, tile)
        return fetch(tok_hbm.at[part], tok.at[part], tok_sem.at[t])

    def ups_copy(t):
        part = pl.ds(t * tile, tile)
        return fetch(ups_hbm.at[part], ups.at[part], ups_sem.at[t])

    gate_copy = fetch(gate_hbm, gate, sem.at[0])
    down_copy = fetch(down_hbm, down, sem.at[1])
    ids_copy = fetch(ids_hbm, ids, sem.at[2])
    up_copy = fetch(up_hbm, up, sem.at[3])
    gate_copy.start()
    down_copy.start()
    ids_copy.start()
    up_copy.start()
    for t in range(TILES):
        tok_copy(t).start()
    frozen_copy = fetch(frozen_hbm, frozen, sem.at[4])
    mine, side = where_ref[0], where_ref[1]
    row_i = lax.broadcasted_iota(jnp.int32, (experts, ranks), 0)
    col_i = lax.broadcasted_iota(jnp.int32, (experts, ranks), 1)
    twice = ((col_i % experts == row_i) & (col_i < 2 * experts)).astype(BF16)
    gate_copy.wait()
    wide_ref[:, ranks:] = nn(gate[...].astype(F32).T.astype(BF16), twice).astype(BF16)
    down_copy.wait()
    wide_ref[:, :ranks] = down[...]
    ids_copy.wait()
    count = jnp.sum((ids[...] != 0).astype(jnp.int32))
    for t in range(TILES):
        part = pl.ds(t * tile, tile)
        tok_copy(t).wait()
        if t == 1:
            for later in range(TILES):
                ups_copy(later).start()
        if t == TILES - 1:
            frozen_copy.start()
        both[part, :] = nn(tok[part, :], wide_ref[...])
    up_copy.wait()
    for t in range(TILES):
        part = pl.ds(t * tile, tile)
        ups_copy(t).wait()
        live = lax.broadcasted_iota(jnp.int32, (tile, 1), 0) + t * tile < count
        ups[part, :] = ups[part, :] * live.astype(F32).astype(BF16)
        back[part, :] = nt(ups[part, :], up[...])
    logits = both[:, ranks:].T[:experts, :]
    shifted = logits - jnp.max(logits, axis=0, keepdims=True)
    powers = jnp.exp(shifted)
    total = jnp.sum(powers, axis=0, keepdims=True)
    prob = powers / total
    logp = shifted - jnp.log(total)
    ent = -jnp.sum(prob * logp, axis=0, keepdims=True)
    alive = (lax.broadcasted_iota(jnp.int32, (1, rows), 1) < count).astype(F32)
    share = alive * prob
    share_ref[...] = share
    big, rest = split(prob)
    mid, small = split(rest)
    parts = jnp.concatenate([big, mid, small], axis=0).T.astype(BF16)
    row_p = lax.broadcasted_iota(jnp.int32, (3 * experts, ranks), 0)
    col_p = lax.broadcasted_iota(jnp.int32, (3 * experts, ranks), 1)
    spread_by = (row_p % experts == col_p // rank).astype(BF16)
    row_g = lax.broadcasted_iota(jnp.int32, (experts, 2 * ranks), 0)
    col_g = lax.broadcasted_iota(jnp.int32, (experts, 2 * ranks), 1)
    group = ((col_g % ranks) // rank == row_g).astype(BF16)
    tasks = []
    for t in range(TILES):
        part = pl.ds(t * tile, tile)
        spread = nn(parts[t * tile : (t + 1) * tile], spread_by)
        low = both[part, :ranks].astype(BF16).astype(F32)
        weighted = (low * spread).astype(BF16)
        weighted_ref[part, :] = weighted
        weighted_t[:, part] = weighted.astype(F32).T.astype(BF16)
        low_grad = (2.0 * spread * back[part, :]).astype(BF16)
        lowgrad_ref[part, :] = low_grad
        left_t[:ranks, part] = low_grad.astype(F32).T.astype(BF16)
        big, small = split(low * back[part, :])
        tasks.append(nt(group, jnp.concatenate([big, small], axis=1).astype(BF16)))
    grad_up[...] = 2.0 * nn(weighted_t[...], ups[...])
    task = 2.0 * jnp.concatenate(tasks, axis=1)
    inner = jnp.sum(prob * task, axis=0, keepdims=True)
    plain = prob * (task - inner) + 50.0 * share * (logp + ent)
    plain_ref[...] = plain
    kinds = experts // 2 + 1
    for kind in range(kinds):
        value = plain if kind == 0 else share * pltpu.roll(prob, experts - kind, 0)
        big, small = split(value)
        at = pl.ds(ranks + 2 * kind * experts, 2 * experts)
        left_t[at, :] = jnp.concatenate([big, small], axis=0).astype(BF16)
    load = jnp.sum(share, axis=1, keepdims=True)
    entropy = jnp.sum(alive * ent, axis=1, keepdims=True)
    lane = lax.broadcasted_iota(jnp.int32, (experts, LANES), 1)
    stats[...] = jnp.where(
        lane < LANES // 2, load, jnp.where(lane < LANES // 4 * 3, entropy, count.astype(F32))
    )
    used = ranks + 2 * kinds * experts
    pairs = width // (2 * LANES)
    depth = pairs.bit_length() - 1
    gate_rows = kinds * experts
    up_rows = ranks * up.shape[1] // (2 * pairs * LANES)
    per = ranks // up_rows
    for pair in range(pairs):
        kept_a, sent_a = spots(mine, pair, side, orders_a, depth)
        kept_b, sent_b = spots(mine, pair, side, orders_b, depth)
        piece = nn(left_t[:used, :], tok[:, pl.ds(pair * 2 * LANES, 2 * LANES)])
        one, two = piece[:, :LANES], piece[:, LANES:]
        gates = []
        for kind in range(kinds):
            at = ranks + 2 * kind * experts
            gates.append(piece[at : at + experts] + piece[at + experts : at + 2 * experts])
        gates = jnp.concatenate(gates, axis=0)
        keep_a[kept_a] = jnp.where(side == 0, one[:ranks], two[:ranks])
        send_a[sent_a] = jnp.where(side == 0, two[:ranks], one[:ranks])
        to = pl.ds(0, gate_rows)
        keep_b[kept_b, to] = jnp.where(side == 0, gates[:, :LANES], gates[:, LANES:])
        send_b[sent_b, to] = jnp.where(side == 0, gates[:, LANES:], gates[:, :LANES])
        keep_b[kept_b, pl.ds(gate_rows, experts)] = stats[...]
        send_b[sent_b, pl.ds(gate_rows, experts)] = stats[...]
        first, second = 2 * pair, 2 * pair + 1
        one = grad_up[pl.ds((first % per) * up_rows, up_rows), pl.ds(first // per * LANES, LANES)]
        two = grad_up[pl.ds((second % per) * up_rows, up_rows), pl.ds(second // per * LANES, LANES)]
        to = pl.ds(gate_rows + experts, up_rows)
        keep_b[kept_b, to] = jnp.where(side == 0, one, two)
        send_b[sent_b, to] = jnp.where(side == 0, two, one)
    frozen_copy.wait()


def in_vmem(*arrays):
    return [pltpu.with_memory_space_constraint(array, VMEM) for array in arrays]


def in_hbm(*arrays):
    return [pltpu.with_memory_space_constraint(array, HBM) for array in arrays]


def local_grads(where, ids, gate_t, down, up, tokens, upstream, frozen, orders_a, orders_b):
    rows, width = tokens.shape
    outs = upstream.shape[1]
    experts, ranks = gate_t.shape[0], down.shape[1]
    pairs = width // (2 * LANES)
    kinds = experts // 2 + 1
    rows_b = (kinds + 1) * experts + ranks * outs // (2 * pairs * LANES)
    return pl.pallas_call(
        functools.partial(local_kernel, orders_a, orders_b),
        out_shape=[
            VMEM((pairs, ranks, LANES), F32),
            VMEM((pairs, ranks, LANES), F32),
            VMEM((pairs, rows_b, LANES), F32),
            VMEM((pairs, rows_b, LANES), F32),
            VMEM((rows, ranks), BF16),
            VMEM((rows, ranks), BF16),
            VMEM((experts, rows), F32),
            VMEM((experts, rows), F32),
            VMEM((width, 2 * ranks), BF16),
            VMEM((rows, outs), BF16),
            VMEM((rows, width), BF16),
            VMEM((ranks, outs), BF16),
            VMEM((width, outs), BF16),
        ],
        in_specs=[pl.BlockSpec(memory_space=SMEM)] + [pl.BlockSpec(memory_space=HBM)] * 7,
        out_specs=[pl.BlockSpec(memory_space=VMEM)] * 13,
        scratch_shapes=[
            VMEM(ids.shape, jnp.int32),
            VMEM((experts, width), BF16),
            VMEM((width, ranks), BF16),
            VMEM((rows, 2 * ranks), F32),
            VMEM((rows, ranks), F32),
            VMEM((2 * ranks, rows), BF16),
            VMEM((ranks, rows), BF16),
            VMEM((ranks, outs), F32),
            VMEM((experts, LANES), F32),
            pltpu.SemaphoreType.DMA((5,)),
            pltpu.SemaphoreType.DMA((TILES,)),
            pltpu.SemaphoreType.DMA((TILES,)),
        ],
        compiler_params=pltpu.CompilerParams(vmem_limit_bytes=20 * MIB),
        cost_estimate=pl.CostEstimate(
            flops=2 * rows * width * 512, bytes_accessed=2 * rows * (width + outs), transcendentals=0
        ),
        name="local_grads",
    )(where, *in_hbm(ids, gate_t, down, up, tokens, upstream, frozen))


def project_kernel(begin, tok, weighted_ref, frozen, up_ref, *rest):
    out_ref, out, out_sem = rest[-3:]
    parts, _, cols = out.shape

    def out_copy(c):
        target = out_ref.at[:, pl.ds((begin + c) * cols, cols)]
        return pltpu.make_async_copy(out.at[c], target, out_sem.at[c])

    for c in range(parts):
        lanes = pl.ds((begin + c) * cols, cols)
        base = nn(tok[...], frozen[:, lanes])
        out[c] = (base + 2.0 * nn(weighted_ref[...], up_ref[:, lanes])).astype(BF16)
        out_copy(c).start()
    for c in range(parts):
        out_copy(c).wait()


def project(tokens, weighted, frozen, up, begin, parts, past):
    rows, width = tokens.shape
    outs, ranks = frozen.shape[1], up.shape[0]
    cols = outs // TILES
    hbm = pl.BlockSpec(memory_space=HBM)
    vmem = pl.BlockSpec(memory_space=VMEM)
    return pl.pallas_call(
        functools.partial(project_kernel, begin),
        out_shape=HBM((rows, outs), BF16),
        in_specs=[vmem] * 4 + [hbm] * len(past),
        out_specs=hbm,
        input_output_aliases={4: 0} if past else {},
        scratch_shapes=[
            VMEM((parts, rows, cols), BF16),
            pltpu.SemaphoreType.DMA((parts,)),
        ],
        compiler_params=pltpu.CompilerParams(vmem_limit_bytes=8 * MIB),
        cost_estimate=pl.CostEstimate(
            flops=2 * rows * cols * parts * (width + ranks),
            bytes_accessed=2 * (rows * width + width * cols * parts + rows * cols * parts),
            transcendentals=0,
        ),
        name="project",
    )(*in_vmem(tokens, weighted, frozen, up), *in_hbm(*past))


def owner_kernel(experts, keep_a, keep_b, recv, own_ref, stats_ref):
    ranks = keep_a.shape[1]
    own_ref[0, :ranks] = keep_a[0] + recv[0, :ranks]
    block = keep_b[0] + recv[0, ranks:]
    kinds = experts // 2 + 1
    at = kinds * experts
    stats = block[at : at + experts]
    stats_ref[...] = stats
    mine = jnp.broadcast_to(stats[:, :1], (experts, LANES))
    total = jnp.zeros((experts, LANES), F32)
    for step in range(1, kinds):
        both = block[step * experts : (step + 1) * experts]
        total = total + both * (mine - pltpu.roll(mine, experts - step, 0))
        if 2 * step != experts:
            total = total + pltpu.roll(both, step, 0) * (mine - pltpu.roll(mine, step, 0))
    scale = 2.0 * experts * 100.0 / stats[:, LANES - 1 :]
    own_ref[0, ranks : ranks + experts] = block[:experts] + scale * total
    own_ref[0, ranks + experts :] = block[at + experts :]


def owner_rows(keep_a, keep_b, recv, experts):
    kinds = experts // 2 + 1
    rows = recv.shape[1] - kinds * experts
    return pl.pallas_call(
        functools.partial(owner_kernel, experts),
        out_shape=[
            jax.ShapeDtypeStruct((1, rows, LANES), F32),
            jax.ShapeDtypeStruct((experts, LANES), F32),
        ],
        compiler_params=pltpu.CompilerParams(vmem_limit_bytes=2 * MIB),
        name="owner_rows",
    )(keep_a, keep_b, recv)


def input_kernel(experts, begin, first, *refs):
    if first:
        masked, lowgrad_ref, plain_ref, share_ref, stats_ref, frozen, wide_ref = refs[:7]
        out_ref, left = refs[7:9]
    else:
        masked, left, frozen, wide_ref = refs[:4]
        out_ref = refs[5]
    out, out_sem = refs[-2:]
    parts, _, cols = out.shape

    def out_copy(c):
        target = out_ref.at[:, pl.ds((begin + c) * cols, cols)]
        return pltpu.make_async_copy(out.at[c], target, out_sem.at[c])

    if first:
        rows, ranks = lowgrad_ref.shape
        weight = stats_ref[:, :1]
        scale = 2.0 * experts * 100.0 / stats_ref[:, LANES - 1 :]
        share = share_ref[...]
        inner = jnp.sum(share * weight, axis=0, keepdims=True)
        value = plain_ref[...] + scale * share * (weight - inner)
        big, small = split(value)
        filler = jnp.zeros((ranks - 2 * experts, rows), F32)
        left[:, :ranks] = lowgrad_ref[...]
        left[:, ranks:] = jnp.concatenate([big, small, filler], axis=0).T.astype(BF16)
    for c in range(parts):
        part = pl.ds((begin + c) * cols, cols)
        out[c] = (nt(masked[...], frozen[part, :]) + nt(left[...], wide_ref[part, :])).astype(BF16)
        out_copy(c).start()
    for c in range(parts):
        out_copy(c).wait()


def input_grads(masked, lefts, frozen, wide, experts, begin, parts, past):
    rows, outs = masked.shape
    width, ranks = frozen.shape[0], wide.shape[1] // 2
    cols = 4 * LANES
    first = not past
    hbm = pl.BlockSpec(memory_space=HBM)
    vmem = pl.BlockSpec(memory_space=VMEM)
    out = HBM((rows, width), BF16)
    return pl.pallas_call(
        functools.partial(input_kernel, experts, begin, first),
        out_shape=[out, VMEM((rows, 2 * ranks), BF16)] if first else out,
        in_specs=[vmem] * (3 + len(lefts)) + [hbm] * len(past),
        out_specs=[hbm, vmem] if first else hbm,
        input_output_aliases={} if first else {4: 0},
        scratch_shapes=[
            VMEM((parts, rows, cols), BF16),
            pltpu.SemaphoreType.DMA((parts,)),
        ],
        compiler_params=pltpu.CompilerParams(vmem_limit_bytes=14 * MIB),
        cost_estimate=pl.CostEstimate(
            flops=2 * rows * cols * parts * (outs + 2 * ranks),
            bytes_accessed=2 * (rows + outs) * cols * parts + 2 * rows * outs,
            transcendentals=0,
        ),
        name="input_grads",
    )(*in_vmem(masked, *lefts, frozen, wide), *in_hbm(*past))


def clip_kernel(orders, experts, limit, where_ref, *refs):
    near, far = refs[:2], refs[2:5]
    stat_own, stat_other = refs[5:7]
    down_hbm, up_hbm, gate_hbm, load_ref, entropy_ref = refs[7:12]
    down, up, gate, squares, down_sem, sem = refs[12:]
    mine, side = where_ref[0], where_ref[1]
    half = near[0].shape[0]
    near = [(ref, spot) for ref in near for spot in range(ref.shape[0])]
    far = [(ref, spot) for ref in far for spot in range(ref.shape[0])]
    depth = (2 * half).bit_length() - 1
    ranks = down.shape[1]
    up_rows = near[0][0].shape[1] - ranks - experts
    per = ranks // up_rows
    blocks = []
    for spot in range(2 * half):
        words = []
        for order in orders:
            word = 0
            for step in range(depth):
                word += ((spot >> (depth - 1 - step)) & 1) << order[step]
            words.append(word)
        base = mine & (2 * half - 1)
        own = base ^ jnp.where(side == 0, words[0], words[1])
        other = base ^ jnp.where(side == 0, words[1], words[0])
        blocks.append((*near[spot], 2 * own + side))
        blocks.append((*far[spot], 2 * other + 1 - side))
    for ref, spot, at in blocks:
        block = ref[spot]
        square = block * block
        squares[at] = jnp.sum(square.reshape(block.shape[0] // 8, 8, LANES), axis=0)
    total = jnp.sum(jnp.sum(squares[...], axis=0), axis=(0, 1), keepdims=True)
    factor = jnp.minimum(1.0, limit / jnp.sqrt(total))
    copies = []
    for number, (ref, spot, at) in enumerate(blocks):
        rows = pl.ds(pl.multiple_of(at * LANES, LANES), LANES)
        down[rows, :] = (ref[spot, :ranks] * factor).T
        copies.append(pltpu.make_async_copy(down.at[rows], down_hbm.at[rows], down_sem.at[number]))
        copies[-1].start()
        gate[:, rows] = ref[spot, ranks : ranks + experts] * factor
        rows = pl.ds(pl.multiple_of(at % per * up_rows, up_rows), up_rows)
        lanes = pl.ds(pl.multiple_of(at // per * LANES, LANES), LANES)
        up[rows, lanes] = ref[spot, ranks + experts :] * factor
    copies.append(pltpu.make_async_copy(up, up_hbm, sem.at[0]))
    copies[-1].start()
    copies.append(pltpu.make_async_copy(gate, gate_hbm, sem.at[1]))
    copies[-1].start()
    stats = jnp.where(side == 0, stat_own[...], stat_other[...])
    stats = stats / stats[:, LANES - 1 :]
    for expert in range(experts):
        load_ref[expert] = jnp.sum(stats[expert : expert + 1, :1])
    entropy_ref[0] = jnp.sum(stats[:1, LANES // 2 : LANES // 2 + 1])
    for copy in copies:
        copy.wait()


def clip_write(where, near, far, stat_own, stat_other, ranks, outs, experts, orders):
    half = near[0].shape[0]
    width = 4 * half * LANES
    limit = math.sqrt(width * ranks + ranks * outs + width * experts)
    vmem = pl.BlockSpec(memory_space=VMEM)
    smem = pl.BlockSpec(memory_space=SMEM)
    hbm = pl.BlockSpec(memory_space=HBM)
    return pl.pallas_call(
        functools.partial(clip_kernel, orders, experts, limit),
        out_shape=[
            HBM((width, ranks), F32),
            HBM((ranks, outs), F32),
            HBM((experts, width), F32),
            jax.ShapeDtypeStruct((experts,), F32),
            jax.ShapeDtypeStruct((1,), F32),
        ],
        in_specs=[smem] + [vmem] * 7,
        out_specs=[hbm] * 3 + [smem] * 2,
        scratch_shapes=[
            VMEM((width, ranks), F32),
            VMEM((ranks, outs), F32),
            VMEM((experts, width), F32),
            VMEM((4 * half, 8, LANES), F32),
            pltpu.SemaphoreType.DMA((4 * half,)),
            pltpu.SemaphoreType.DMA((2,)),
        ],
        compiler_params=pltpu.CompilerParams(vmem_limit_bytes=8 * MIB),
        name="clip_write",
    )(where, *in_vmem(*near, *far, stat_own, stat_other))


def swap(array, masks):
    size = lax.axis_size("dp")
    return lax.ppermute(array, "dp", [(i, i ^ masks[i & 1]) for i in range(size)])


def halve(keep, recv):
    half = keep.shape[0] // 2
    send = keep[half:] + recv[half:]
    return keep[:half] + recv[:half], send


def on_device(token_ids, tokens, frozen, down, up, gate, upstream):
    experts = gate.shape[1]
    outs = frozen.shape[1]
    rows = tokens.shape[0]
    size = lax.axis_size("dp")
    bits = size.bit_length() - 2
    depth = (tokens.shape[1] // (2 * LANES)).bit_length() - 1
    rest = tuple(range(2, bits))
    orders_a = ((0, 1) + rest, (1, 0) + rest)
    orders_b = ((2, 0, 1) + rest[1:], (2, 1, 0) + rest[1:])
    me = lax.axis_index("dp")
    where = jnp.stack([me >> 1, me & 1]).astype(jnp.int32)
    ids = token_ids.reshape(rows // LANES, LANES)
    orders_g = orders_a
    masks_g = [(2 << orders_g[0][s], 2 << orders_g[1][s]) for s in range(bits)]
    masks_a = [(2 << orders_a[0][s], 2 << orders_a[1][s]) for s in range(bits)]
    masks_b = [(2 << orders_b[0][s], 2 << orders_b[1][s]) for s in range(bits)]

    keep_a, send_a, keep_b, send_b, weighted, low_grad, plain, share, wide, masked, tok, up_v, near = (
        local_grads(where, ids, gate.T, down, up, tokens, upstream, frozen, orders_a, orders_b)
    )
    split_at = keep_a.shape[1]
    filled = ()
    begin = 0
    for step in range(-1, bits):
        if step >= depth:
            keep_b = send_b = keep_b + recv_b
            keep_a = send_a = keep_a + recv_a
        elif step >= 0:
            keep_b, send_b = halve(keep_b, recv_b)
            keep_a, send_a = halve(keep_a, recv_a)
        parts = AHEAD[step + 1] if step + 1 < len(AHEAD) else 0
        if parts:
            weighted, send_a, send_b, filled = lax.optimization_barrier(
                (weighted, send_a, send_b, filled)
            )
            filled = (project(tok, weighted, near, up_v, begin, parts, filled),)
            begin += parts
        mask_a, mask_b = ((1, 1), (1, 1)) if step < 0 else (masks_a[step], masks_b[step])
        if step >= 0 and mask_a == mask_b:
            recv = swap(jnp.concatenate([send_a, send_b], axis=1), mask_a)
            recv_a, recv_b = recv[:, :split_at], recv[:, split_at:]
        else:
            recv_b = swap(send_b, mask_b)
            recv_a = swap(send_a, mask_a)
        if parts:
            recv_a, recv_b, filled = lax.optimization_barrier((recv_a, recv_b, filled))
    projected = filled[0]
    own, stats = owner_rows(keep_a, keep_b, recv, experts)
    lefts = (low_grad, plain, share, stats)
    filled = ()
    begin = 0
    tiles = tokens.shape[1] // (4 * LANES)
    turns = tuple(reversed(range(depth)))
    for turn, step in enumerate(turns):
        lefts, own, filled = lax.optimization_barrier((lefts, own, filled))
        last = turn == depth - 1
        parts = tiles - begin if last else CHUNKS[turn]
        if parts:
            made = input_grads(masked, lefts, near, wide, experts, begin, parts, filled)
            begin += parts
            if isinstance(made, (list, tuple)):
                filled, lefts = (made[0],), (made[1],)
            else:
                filled = (made,)
        if turn == depth - 2:
            far = (swap(own, (1, 1)),)
            recv = swap(own, masks_g[step])
        else:
            recv = swap(own, masks_g[step])
        if last:
            far += (swap(own[own.shape[0] // 2 :], (1, 1)),)
            stat_other = swap(stats, (1, 1))
        recv, filled = lax.optimization_barrier((recv, filled))
        if not last:
            own = jnp.concatenate([own, recv], axis=0)
    input_grad = filled[0]
    far += (swap(recv, (1, 1)),)
    clipped_down, clipped_up, clipped_gate, load, entropy = clip_write(
        where, (own, recv), far, stats, stat_other, split_at, outs, experts, orders_g
    )
    return (
        projected,
        input_grad,
        clipped_down,
        clipped_up,
        clipped_gate.T,
        load,
        entropy.reshape(()),
    )


def solution(mesh):
    placed = (P("dp"), P("dp", None), P(), P(), P(), P(), P("dp", None))
    return jax.shard_map(
        on_device,
        mesh=mesh,
        in_specs=placed,
        out_specs=(P("dp", None), P("dp", None), P(), P(), P(), P(), P()),
        check_vma=False,
    )
```

```python
import functools
import math

import jax
import jax.numpy as jnp
from jax import lax
from jax.experimental import pallas as pl
from jax.experimental.pallas import tpu as pltpu
from jax.sharding import PartitionSpec as P


F32 = jnp.float32
BF16 = jnp.bfloat16
LANES = 128
TILES = 4
AHEAD = (1, 1, 1, 1)
CHUNKS = (1, 2)
VMEM = pltpu.VMEM
SMEM = pltpu.SMEM
HBM = pltpu.HBM
MIB = 1024 * 1024


def nn(a, b):
    return lax.dot_general(a, b, (((1,), (0,)), ((), ())), preferred_element_type=F32)


def nt(a, b):
    return lax.dot_general(a, b, (((1,), (1,)), ((), ())), preferred_element_type=F32)


def split(x):
    upper = x.astype(BF16).astype(F32)
    return upper, x - upper


def place(word, order, depth):
    spot = 0
    for step in range(depth):
        spot = spot + (((word >> order[step]) & 1) << (depth - 1 - step))
    return spot


def spots(mine, pair, side, orders, depth):
    word = (mine ^ pair) & ((1 << depth) - 1)
    first = place(word, orders[0], depth)
    second = place(word, orders[1], depth)
    kept = jnp.where(side == 0, first, second)
    sent = jnp.where(side == 0, second, first)
    return kept, sent


def local_kernel(
    orders_a, orders_b, where_ref, ids_hbm, gate_hbm, down_hbm, up_hbm, tok_hbm, ups_hbm, frozen_hbm,
    keep_a, send_a, keep_b, send_b, weighted_ref, lowgrad_ref, plain_ref, share_ref, wide_ref, ups,
    tok, up, frozen, ids, gate, down, both, back, left_t, weighted_t, grad_up, stats, sem, tok_sem, ups_sem,
):
    rows, width = tok.shape
    experts, ranks = gate.shape[0], down.shape[1]
    rank = ranks // experts
    tile = rows // TILES

    def fetch(source, target, flag):
        return pltpu.make_async_copy(source, target, flag)

    def tok_copy(t):
        part = pl.ds(t * tile, tile)
        return fetch(tok_hbm.at[part], tok.at[part], tok_sem.at[t])

    def ups_copy(t):
        part = pl.ds(t * tile, tile)
        return fetch(ups_hbm.at[part], ups.at[part], ups_sem.at[t])

    gate_copy = fetch(gate_hbm, gate, sem.at[0])
    down_copy = fetch(down_hbm, down, sem.at[1])
    ids_copy = fetch(ids_hbm, ids, sem.at[2])
    up_copy = fetch(up_hbm, up, sem.at[3])
    gate_copy.start()
    down_copy.start()
    ids_copy.start()
    up_copy.start()
    for t in range(TILES):
        tok_copy(t).start()
    frozen_copy = fetch(frozen_hbm, frozen, sem.at[4])
    mine, side = where_ref[0], where_ref[1]
    row_i = lax.broadcasted_iota(jnp.int32, (experts, ranks), 0)
    col_i = lax.broadcasted_iota(jnp.int32, (experts, ranks), 1)
    twice = ((col_i % experts == row_i) & (col_i < 2 * experts)).astype(BF16)
    gate_copy.wait()
    wide_ref[:, ranks:] = nn(gate[...].astype(F32).T.astype(BF16), twice).astype(BF16)
    down_copy.wait()
    wide_ref[:, :ranks] = down[...]
    for t in range(TILES):
        part = pl.ds(t * tile, tile)
        tok_copy(t).wait()
        if t == 1:
            for later in range(TILES):
                ups_copy(later).start()
        if t == TILES - 1:
            frozen_copy.start()
        both[part, :] = nn(tok[part, :], wide_ref[...])
    ids_copy.wait()
    count = jnp.sum((ids[...] != 0).astype(jnp.int32))
    up_copy.wait()
    for t in range(TILES):
        part = pl.ds(t * tile, tile)
        ups_copy(t).wait()
        live = lax.broadcasted_iota(jnp.int32, (tile, 1), 0) + t * tile < count
        ups[part, :] = ups[part, :] * live.astype(F32).astype(BF16)
    back[...] = nt(ups[...], up[...])
    logits = both[:, ranks:].T[:experts, :]
    shifted = logits - jnp.max(logits, axis=0, keepdims=True)
    powers = jnp.exp(shifted)
    total = jnp.sum(powers, axis=0, keepdims=True)
    prob = powers / total
    logp = shifted - jnp.log(total)
    ent = -jnp.sum(prob * logp, axis=0, keepdims=True)
    alive = (lax.broadcasted_iota(jnp.int32, (1, rows), 1) < count).astype(F32)
    share = alive * prob
    share_ref[...] = share
    big, rest = split(prob)
    mid, small = split(rest)
    parts = jnp.concatenate([big, mid, small], axis=0).T.astype(BF16)
    row_p = lax.broadcasted_iota(jnp.int32, (3 * experts, ranks), 0)
    col_p = lax.broadcasted_iota(jnp.int32, (3 * experts, ranks), 1)
    spread_by = (row_p % experts == col_p // rank).astype(BF16)
    row_g = lax.broadcasted_iota(jnp.int32, (experts, 2 * ranks), 0)
    col_g = lax.broadcasted_iota(jnp.int32, (experts, 2 * ranks), 1)
    group = ((col_g % ranks) // rank == row_g).astype(BF16)
    tasks = []
    for t in range(TILES):
        part = pl.ds(t * tile, tile)
        spread = nn(parts[t * tile : (t + 1) * tile], spread_by)
        low = both[part, :ranks].astype(BF16).astype(F32)
        weighted = (low * spread).astype(BF16)
        weighted_ref[part, :] = weighted
        weighted_t[:, part] = weighted.astype(F32).T.astype(BF16)
        low_grad = (2.0 * spread * back[part, :]).astype(BF16)
        lowgrad_ref[part, :] = low_grad
        left_t[:ranks, part] = low_grad.astype(F32).T.astype(BF16)
        big, small = split(low * back[part, :])
        tasks.append(nt(group, jnp.concatenate([big, small], axis=1).astype(BF16)))
    grad_up[...] = 2.0 * nn(weighted_t[...], ups[...])
    task = 2.0 * jnp.concatenate(tasks, axis=1)
    inner = jnp.sum(prob * task, axis=0, keepdims=True)
    plain = prob * (task - inner) + 50.0 * share * (logp + ent)
    plain_ref[...] = plain
    kinds = experts // 2 + 1
    for kind in range(kinds):
        value = plain if kind == 0 else share * pltpu.roll(prob, experts - kind, 0)
        big, small = split(value)
        at = pl.ds(ranks + 2 * kind * experts, 2 * experts)
        left_t[at, :] = jnp.concatenate([big, small], axis=0).astype(BF16)
    load = jnp.sum(share, axis=1, keepdims=True)
    entropy = jnp.sum(alive * ent, axis=1, keepdims=True)
    half = experts // 2
    lane = lax.broadcasted_iota(jnp.int32, (half, LANES), 1)
    pair_load = jnp.where(lane < LANES // 4, load[:half], load[half:])
    rest = jnp.where(lane < LANES // 4 * 3, entropy, count.astype(F32))
    stats[...] = jnp.where(lane < LANES // 2, pair_load, rest)
    used = ranks + 2 * kinds * experts
    pairs = width // (2 * LANES)
    depth = pairs.bit_length() - 1
    gate_rows = kinds * experts
    up_rows = ranks * up.shape[1] // (2 * pairs * LANES)
    per = ranks // up_rows
    for pair in range(pairs):
        kept_a, sent_a = spots(mine, pair, side, orders_a, depth)
        kept_b, sent_b = spots(mine, pair, side, orders_b, depth)
        piece = nn(left_t[:used, :], tok[:, pl.ds(pair * 2 * LANES, 2 * LANES)])
        one, two = piece[:, :LANES], piece[:, LANES:]
        gates = []
        for kind in range(kinds):
            at = ranks + 2 * kind * experts
            gates.append(piece[at : at + experts] + piece[at + experts : at + 2 * experts])
        gates = jnp.concatenate(gates, axis=0)
        keep_a[kept_a] = jnp.where(side == 0, one[:ranks], two[:ranks])
        send_a[sent_a] = jnp.where(side == 0, two[:ranks], one[:ranks])
        to = pl.ds(0, gate_rows)
        keep_b[kept_b, to] = jnp.where(side == 0, gates[:, :LANES], gates[:, LANES:])
        send_b[sent_b, to] = jnp.where(side == 0, gates[:, LANES:], gates[:, :LANES])
        keep_b[kept_b, pl.ds(gate_rows - half, half)] = stats[...]
        send_b[sent_b, pl.ds(gate_rows - half, half)] = stats[...]
        first, second = 2 * pair, 2 * pair + 1
        one = grad_up[pl.ds((first % per) * up_rows, up_rows), pl.ds(first // per * LANES, LANES)]
        two = grad_up[pl.ds((second % per) * up_rows, up_rows), pl.ds(second // per * LANES, LANES)]
        to = pl.ds(gate_rows, up_rows)
        keep_b[kept_b, to] = jnp.where(side == 0, one, two)
        send_b[sent_b, to] = jnp.where(side == 0, two, one)
    frozen_copy.wait()


def in_vmem(*arrays):
    return [pltpu.with_memory_space_constraint(array, VMEM) for array in arrays]


def in_hbm(*arrays):
    return [pltpu.with_memory_space_constraint(array, HBM) for array in arrays]


def local_grads(where, ids, gate_t, down, up, tokens, upstream, frozen, orders_a, orders_b):
    rows, width = tokens.shape
    outs = upstream.shape[1]
    experts, ranks = gate_t.shape[0], down.shape[1]
    pairs = width // (2 * LANES)
    kinds = experts // 2 + 1
    rows_b = kinds * experts + ranks * outs // (2 * pairs * LANES)
    return pl.pallas_call(
        functools.partial(local_kernel, orders_a, orders_b),
        out_shape=[
            VMEM((pairs, ranks, LANES), F32),
            VMEM((pairs, ranks, LANES), F32),
            VMEM((pairs, rows_b, LANES), F32),
            VMEM((pairs, rows_b, LANES), F32),
            VMEM((rows, ranks), BF16),
            VMEM((rows, ranks), BF16),
            VMEM((experts, rows), F32),
            VMEM((experts, rows), F32),
            VMEM((width, 2 * ranks), BF16),
            VMEM((rows, outs), BF16),
            VMEM((rows, width), BF16),
            VMEM((ranks, outs), BF16),
            VMEM((width, outs), BF16),
        ],
        in_specs=[pl.BlockSpec(memory_space=SMEM)] + [pl.BlockSpec(memory_space=HBM)] * 7,
        out_specs=[pl.BlockSpec(memory_space=VMEM)] * 13,
        scratch_shapes=[
            VMEM(ids.shape, jnp.int32),
            VMEM((experts, width), BF16),
            VMEM((width, ranks), BF16),
            VMEM((rows, 2 * ranks), F32),
            VMEM((rows, ranks), F32),
            VMEM((2 * ranks, rows), BF16),
            VMEM((ranks, rows), BF16),
            VMEM((ranks, outs), F32),
            VMEM((experts // 2, LANES), F32),
            pltpu.SemaphoreType.DMA((5,)),
            pltpu.SemaphoreType.DMA((TILES,)),
            pltpu.SemaphoreType.DMA((TILES,)),
        ],
        compiler_params=pltpu.CompilerParams(vmem_limit_bytes=20 * MIB),
        cost_estimate=pl.CostEstimate(
            flops=2 * rows * width * 512, bytes_accessed=2 * rows * (width + outs), transcendentals=0
        ),
        name="local_grads",
    )(where, *in_hbm(ids, gate_t, down, up, tokens, upstream, frozen))


def project_kernel(begin, tok, weighted_ref, frozen, up_ref, *rest):
    out_ref, out, out_sem = rest[-3:]
    parts, _, cols = out.shape

    def out_copy(c):
        target = out_ref.at[:, pl.ds((begin + c) * cols, cols)]
        return pltpu.make_async_copy(out.at[c], target, out_sem.at[c])

    for c in range(parts):
        lanes = pl.ds((begin + c) * cols, cols)
        base = nn(tok[...], frozen[:, lanes])
        out[c] = (base + 2.0 * nn(weighted_ref[...], up_ref[:, lanes])).astype(BF16)
        out_copy(c).start()
    for c in range(parts):
        out_copy(c).wait()


def project(tokens, weighted, frozen, up, begin, parts, past):
    rows, width = tokens.shape
    outs, ranks = frozen.shape[1], up.shape[0]
    cols = outs // TILES
    hbm = pl.BlockSpec(memory_space=HBM)
    vmem = pl.BlockSpec(memory_space=VMEM)
    return pl.pallas_call(
        functools.partial(project_kernel, begin),
        out_shape=HBM((rows, outs), BF16),
        in_specs=[vmem] * 4 + [hbm] * len(past),
        out_specs=hbm,
        input_output_aliases={4: 0} if past else {},
        scratch_shapes=[
            VMEM((parts, rows, cols), BF16),
            pltpu.SemaphoreType.DMA((parts,)),
        ],
        compiler_params=pltpu.CompilerParams(vmem_limit_bytes=8 * MIB),
        cost_estimate=pl.CostEstimate(
            flops=2 * rows * cols * parts * (width + ranks),
            bytes_accessed=2 * (rows * width + width * cols * parts + rows * cols * parts),
            transcendentals=0,
        ),
        name="project",
    )(*in_vmem(tokens, weighted, frozen, up), *in_hbm(*past))


def owner_kernel(experts, keep_a, keep_b, recv, own_ref, stats_ref):
    count, ranks = keep_a.shape[:2]
    half = experts // 2
    at = (half + 1) * experts
    lane = lax.broadcasted_iota(jnp.int32, (experts, LANES), 1)
    shape = (half, LANES)
    for spot in range(count):
        own_ref[spot, :ranks] = keep_a[spot] + recv[spot, :ranks]
        block = keep_b[spot] + recv[spot, ranks:]
        stats = block[at - half : at]
        first = jnp.broadcast_to(stats[:, :1], shape)
        second = jnp.broadcast_to(stats[:, LANES // 4 : LANES // 4 + 1], shape)
        mine = jnp.concatenate([first, second], axis=0)
        if spot == 0:
            stats_ref[...] = jnp.where(lane < LANES // 2, mine, stats[:1])
        total = jnp.zeros((experts, LANES), F32)
        for step in range(1, half):
            both = block[step * experts : (step + 1) * experts]
            total = total + both * (mine - pltpu.roll(mine, experts - step, 0))
            total = total + pltpu.roll(both, step, 0) * (mine - pltpu.roll(mine, step, 0))
        both = block[at - experts : at - half]
        both = jnp.concatenate([both, both], axis=0)
        total = total + both * (mine - pltpu.roll(mine, half, 0))
        scale = 2.0 * experts * 100.0 / stats[:1, LANES - 1 :]
        own_ref[spot, ranks : ranks + experts] = block[:experts] + scale * total
        own_ref[spot, ranks + experts :] = block[at:]


def owner_rows(keep_a, keep_b, recv, experts):
    rows = recv.shape[1] - experts // 2 * experts
    return pl.pallas_call(
        functools.partial(owner_kernel, experts),
        out_shape=[
            jax.ShapeDtypeStruct((keep_a.shape[0], rows, LANES), F32),
            jax.ShapeDtypeStruct((experts, LANES), F32),
        ],
        compiler_params=pltpu.CompilerParams(vmem_limit_bytes=2 * MIB),
        name="owner_rows",
    )(keep_a, keep_b, recv)


def input_kernel(experts, begin, first, *refs):
    if first:
        masked, lowgrad_ref, plain_ref, share_ref, stats_ref, frozen, wide_ref = refs[:7]
        out_ref, left = refs[7:9]
    else:
        masked, left, frozen, wide_ref = refs[:4]
        out_ref = refs[5]
    out, out_sem = refs[-2:]
    parts, _, cols = out.shape

    def out_copy(c):
        target = out_ref.at[:, pl.ds((begin + c) * cols, cols)]
        return pltpu.make_async_copy(out.at[c], target, out_sem.at[c])

    if first:
        rows, ranks = lowgrad_ref.shape
        weight = stats_ref[:, :1]
        scale = 2.0 * experts * 100.0 / stats_ref[:, LANES - 1 :]
        share = share_ref[...]
        inner = jnp.sum(share * weight, axis=0, keepdims=True)
        value = plain_ref[...] + scale * share * (weight - inner)
        big, small = split(value)
        filler = jnp.zeros((ranks - 2 * experts, rows), F32)
        left[:, :ranks] = lowgrad_ref[...]
        left[:, ranks:] = jnp.concatenate([big, small, filler], axis=0).T.astype(BF16)
    for c in range(parts):
        part = pl.ds((begin + c) * cols, cols)
        out[c] = (nt(masked[...], frozen[part, :]) + nt(left[...], wide_ref[part, :])).astype(BF16)
        out_copy(c).start()
    for c in range(parts):
        out_copy(c).wait()


def input_grads(masked, lefts, frozen, wide, experts, begin, parts, past):
    rows, outs = masked.shape
    width, ranks = frozen.shape[0], wide.shape[1] // 2
    cols = 4 * LANES
    first = not past
    hbm = pl.BlockSpec(memory_space=HBM)
    vmem = pl.BlockSpec(memory_space=VMEM)
    out = HBM((rows, width), BF16)
    return pl.pallas_call(
        functools.partial(input_kernel, experts, begin, first),
        out_shape=[out, VMEM((rows, 2 * ranks), BF16)] if first else out,
        in_specs=[vmem] * (3 + len(lefts)) + [hbm] * len(past),
        out_specs=[hbm, vmem] if first else hbm,
        input_output_aliases={} if first else {4: 0},
        scratch_shapes=[
            VMEM((parts, rows, cols), BF16),
            pltpu.SemaphoreType.DMA((parts,)),
        ],
        compiler_params=pltpu.CompilerParams(vmem_limit_bytes=14 * MIB),
        cost_estimate=pl.CostEstimate(
            flops=2 * rows * cols * parts * (outs + 2 * ranks),
            bytes_accessed=2 * (rows + outs) * cols * parts + 2 * rows * outs,
            transcendentals=0,
        ),
        name="input_grads",
    )(*in_vmem(masked, *lefts, frozen, wide), *in_hbm(*past))


def clip_kernel(orders, experts, limit, where_ref, *refs):
    near, far = refs[:2], refs[2:5]
    stat_own, stat_other = refs[5:7]
    down_hbm, up_hbm, gate_hbm, load_ref, entropy_ref = refs[7:12]
    down, up, gate, squares, down_sem, sem = refs[12:]
    mine, side = where_ref[0], where_ref[1]
    half = near[0].shape[0]
    near = [(ref, spot) for ref in near for spot in range(ref.shape[0])]
    far = [(ref, spot) for ref in far for spot in range(ref.shape[0])]
    depth = (2 * half).bit_length() - 1
    ranks = down.shape[1]
    up_rows = near[0][0].shape[1] - ranks - experts
    per = ranks // up_rows
    blocks = []
    for spot in range(2 * half):
        words = []
        for order in orders:
            word = 0
            for step in range(depth):
                word += ((spot >> (depth - 1 - step)) & 1) << order[step]
            words.append(word)
        base = mine & (2 * half - 1)
        own = base ^ jnp.where(side == 0, words[0], words[1])
        other = base ^ jnp.where(side == 0, words[1], words[0])
        blocks.append((*near[spot], 2 * own + side))
        blocks.append((*far[spot], 2 * other + 1 - side))
    for ref, spot, at in blocks:
        block = ref[spot]
        square = block * block
        squares[at] = jnp.sum(square.reshape(block.shape[0] // 8, 8, LANES), axis=0)
    total = jnp.sum(jnp.sum(squares[...], axis=0), axis=(0, 1), keepdims=True)
    factor = jnp.minimum(1.0, limit / jnp.sqrt(total))
    copies = []
    for number, (ref, spot, at) in enumerate(blocks):
        rows = pl.ds(pl.multiple_of(at * LANES, LANES), LANES)
        down[rows, :] = (ref[spot, :ranks] * factor).T
        copies.append(pltpu.make_async_copy(down.at[rows], down_hbm.at[rows], down_sem.at[number]))
        copies[-1].start()
        gate[:, rows] = ref[spot, ranks : ranks + experts] * factor
        rows = pl.ds(pl.multiple_of(at % per * up_rows, up_rows), up_rows)
        lanes = pl.ds(pl.multiple_of(at // per * LANES, LANES), LANES)
        up[rows, lanes] = ref[spot, ranks + experts :] * factor
    copies.append(pltpu.make_async_copy(up, up_hbm, sem.at[0]))
    copies[-1].start()
    copies.append(pltpu.make_async_copy(gate, gate_hbm, sem.at[1]))
    copies[-1].start()
    stats = jnp.where(side == 0, stat_own[...], stat_other[...])
    stats = stats / stats[:, LANES - 1 :]
    for expert in range(experts):
        load_ref[expert] = jnp.sum(stats[expert : expert + 1, :1])
    entropy_ref[0] = jnp.sum(stats[:1, LANES // 2 : LANES // 2 + 1])
    for copy in copies:
        copy.wait()


def clip_write(where, near, far, stat_own, stat_other, ranks, outs, experts, orders):
    half = near[0].shape[0]
    width = 4 * half * LANES
    limit = math.sqrt(width * ranks + ranks * outs + width * experts)
    vmem = pl.BlockSpec(memory_space=VMEM)
    smem = pl.BlockSpec(memory_space=SMEM)
    hbm = pl.BlockSpec(memory_space=HBM)
    return pl.pallas_call(
        functools.partial(clip_kernel, orders, experts, limit),
        out_shape=[
            HBM((width, ranks), F32),
            HBM((ranks, outs), F32),
            HBM((experts, width), F32),
            jax.ShapeDtypeStruct((experts,), F32),
            jax.ShapeDtypeStruct((1,), F32),
        ],
        in_specs=[smem] + [vmem] * 7,
        out_specs=[hbm] * 3 + [smem] * 2,
        scratch_shapes=[
            VMEM((width, ranks), F32),
            VMEM((ranks, outs), F32),
            VMEM((experts, width), F32),
            VMEM((4 * half, 8, LANES), F32),
            pltpu.SemaphoreType.DMA((4 * half,)),
            pltpu.SemaphoreType.DMA((2,)),
        ],
        compiler_params=pltpu.CompilerParams(vmem_limit_bytes=8 * MIB),
        name="clip_write",
    )(where, *in_vmem(*near, *far, stat_own, stat_other))


def swap(array, masks):
    size = lax.axis_size("dp")
    return lax.ppermute(array, "dp", [(i, i ^ masks[i & 1]) for i in range(size)])


def halve(keep, recv):
    half = keep.shape[0] // 2
    send = keep[half:] + recv[half:]
    return keep[:half] + recv[:half], send


def on_device(token_ids, tokens, frozen, down, up, gate, upstream):
    experts = gate.shape[1]
    outs = frozen.shape[1]
    rows = tokens.shape[0]
    size = lax.axis_size("dp")
    bits = size.bit_length() - 2
    depth = (tokens.shape[1] // (2 * LANES)).bit_length() - 1
    rest = tuple(range(2, bits))
    orders_a = ((0, 1) + rest, (1, 0) + rest)
    orders_b = ((2, 0, 1) + rest[1:], (2, 1, 0) + rest[1:])
    me = lax.axis_index("dp")
    where = jnp.stack([me >> 1, me & 1]).astype(jnp.int32)
    ids = token_ids.reshape(rows // LANES, LANES)
    orders_g = orders_a
    masks_g = [(2 << orders_g[0][s], 2 << orders_g[1][s]) for s in range(bits)]
    masks_a = [(2 << orders_a[0][s], 2 << orders_a[1][s]) for s in range(bits)]
    masks_b = [(2 << orders_b[0][s], 2 << orders_b[1][s]) for s in range(bits)]

    keep_a, send_a, keep_b, send_b, weighted, low_grad, plain, share, wide, masked, tok, up_v, near = (
        local_grads(where, ids, gate.T, down, up, tokens, upstream, frozen, orders_a, orders_b)
    )
    split_at = keep_a.shape[1]
    filled = ()
    begin = 0
    for step in range(-1, bits):
        if step >= depth - 1:
            keep_b = send_b = keep_b + recv_b
            keep_a = send_a = keep_a + recv_a
            if step == depth - 1:
                send_b = jnp.concatenate([send_b[1:], send_b[:1]], axis=0)
                send_a = jnp.concatenate([send_a[1:], send_a[:1]], axis=0)
        elif step >= 0:
            keep_b, send_b = halve(keep_b, recv_b)
            keep_a, send_a = halve(keep_a, recv_a)
        parts = AHEAD[step + 1] if step + 1 < len(AHEAD) else 0
        if parts:
            weighted, send_a, send_b, filled = lax.optimization_barrier(
                (weighted, send_a, send_b, filled)
            )
            filled = (project(tok, weighted, near, up_v, begin, parts, filled),)
            begin += parts
        mask_a, mask_b = ((1, 1), (1, 1)) if step < 0 else (masks_a[step], masks_b[step])
        if step >= 0 and mask_a == mask_b:
            recv = swap(jnp.concatenate([send_a, send_b], axis=1), mask_a)
            recv_a, recv_b = recv[:, :split_at], recv[:, split_at:]
        else:
            recv_b = swap(send_b, mask_b)
            recv_a = swap(send_a, mask_a)
        if parts:
            recv_a, recv_b, filled = lax.optimization_barrier((recv_a, recv_b, filled))
    projected = filled[0]
    own, stats = owner_rows(keep_a, keep_b, recv, experts)
    lefts = (low_grad, plain, share, stats)
    filled = ()
    begin = 0
    tiles = tokens.shape[1] // (4 * LANES)
    turns = tuple(reversed(range(depth - 1)))
    for turn, step in enumerate(turns):
        lefts, own, filled = lax.optimization_barrier((lefts, own, filled))
        last = turn == len(turns) - 1
        parts = tiles - begin if last else CHUNKS[turn]
        if parts:
            made = input_grads(masked, lefts, near, wide, experts, begin, parts, filled)
            begin += parts
            if isinstance(made, (list, tuple)):
                filled, lefts = (made[0],), (made[1],)
            else:
                filled = (made,)
        if turn == len(turns) - 2:
            far = (swap(own, (1, 1)),)
            recv = swap(own, masks_g[step])
        else:
            recv = swap(own, masks_g[step])
        if last:
            far += (swap(own[own.shape[0] // 2 :], (1, 1)),)
            stat_other = swap(stats, (1, 1))
        recv, filled = lax.optimization_barrier((recv, filled))
        if not last:
            own = jnp.concatenate([own, recv], axis=0)
    input_grad = filled[0]
    far += (swap(recv, (1, 1)),)
    clipped_down, clipped_up, clipped_gate, load, entropy = clip_write(
        where, (own, recv), far, stats, stat_other, split_at, outs, experts, orders_g
    )
    return (
        projected,
        input_grad,
        clipped_down,
        clipped_up,
        clipped_gate.T,
        load,
        entropy.reshape(()),
    )


def solution(mesh):
    placed = (P("dp"), P("dp", None), P(), P(), P(), P(), P("dp", None))
    return jax.shard_map(
        on_device,
        mesh=mesh,
        in_specs=placed,
        out_specs=(P("dp", None), P("dp", None), P(), P(), P(), P(), P()),
        check_vma=False,
    )
```

```python
import functools
import math

import jax
import jax.numpy as jnp
from jax import lax
from jax.experimental import pallas as pl
from jax.experimental.pallas import tpu as pltpu
from jax.sharding import PartitionSpec as P


F32 = jnp.float32
BF16 = jnp.bfloat16
LANES = 128
TILES = 4
AHEAD = (1, 1, 1, 1)
CHUNKS = (1, 2)
VMEM = pltpu.VMEM
SMEM = pltpu.SMEM
HBM = pltpu.HBM
MIB = 1024 * 1024


def nn(a, b):
    return lax.dot_general(a, b, (((1,), (0,)), ((), ())), preferred_element_type=F32)


def nt(a, b):
    return lax.dot_general(a, b, (((1,), (1,)), ((), ())), preferred_element_type=F32)


def split(x):
    upper = x.astype(BF16).astype(F32)
    return upper, x - upper


def place(word, order, depth):
    spot = 0
    for step in range(depth):
        spot = spot + (((word >> order[step]) & 1) << (depth - 1 - step))
    return spot


def spots(mine, pair, side, orders, depth):
    word = (mine ^ pair) & ((1 << depth) - 1)
    first = place(word, orders[0], depth)
    second = place(word, orders[1], depth)
    kept = jnp.where(side == 0, first, second)
    sent = jnp.where(side == 0, second, first)
    return kept, sent


def local_kernel(
    orders_a, orders_b, where_ref, ids_hbm, gate_hbm, down_hbm, up_hbm, tok_hbm, ups_hbm, frozen_hbm,
    keep_a, send_a, keep_b, send_b, weighted_ref, lowgrad_ref, plain_ref, share_ref, wide_ref, ups,
    tok, up, frozen, ids, gate, down, both, left_t, weighted_t, grad_up, stats, sem, tok_sem, ups_sem,
):
    rows, width = tok.shape
    experts, ranks = gate.shape[0], down.shape[1]
    rank = ranks // experts
    tile = rows // TILES

    def fetch(source, target, flag):
        return pltpu.make_async_copy(source, target, flag)

    def tok_copy(t):
        part = pl.ds(t * tile, tile)
        return fetch(tok_hbm.at[part], tok.at[part], tok_sem.at[t])

    def ups_copy(t):
        part = pl.ds(t * tile, tile)
        return fetch(ups_hbm.at[part], ups.at[part], ups_sem.at[t])

    gate_copy = fetch(gate_hbm, gate, sem.at[0])
    down_copy = fetch(down_hbm, down, sem.at[1])
    ids_copy = fetch(ids_hbm, ids, sem.at[2])
    up_copy = fetch(up_hbm, up, sem.at[3])
    gate_copy.start()
    down_copy.start()
    ids_copy.start()
    up_copy.start()
    for t in range(TILES):
        tok_copy(t).start()
        ups_copy(t).start()
    frozen_copy = fetch(frozen_hbm, frozen, sem.at[4])
    mine, side = where_ref[0], where_ref[1]
    row_i = lax.broadcasted_iota(jnp.int32, (experts, ranks), 0)
    col_i = lax.broadcasted_iota(jnp.int32, (experts, ranks), 1)
    twice = ((col_i % experts == row_i) & (col_i < 2 * experts)).astype(BF16)
    gate_copy.wait()
    wide_ref[:, ranks:] = nn(gate[...].astype(F32).T.astype(BF16), twice).astype(BF16)
    down_copy.wait()
    wide_ref[:, :ranks] = down[...]
    ids_copy.wait()
    count = jnp.sum((ids[...] != 0).astype(jnp.int32))
    up_copy.wait()
    row_p = lax.broadcasted_iota(jnp.int32, (3 * experts, ranks), 0)
    col_p = lax.broadcasted_iota(jnp.int32, (3 * experts, ranks), 1)
    spread_by = (row_p % experts == col_p // rank).astype(BF16)
    row_g = lax.broadcasted_iota(jnp.int32, (experts, 2 * ranks), 0)
    col_g = lax.broadcasted_iota(jnp.int32, (experts, 2 * ranks), 1)
    group = ((col_g % ranks) // rank == row_g).astype(BF16)
    kinds = experts // 2 + 1

    def finish(t):
        part = pl.ds(t * tile, tile)
        live = lax.broadcasted_iota(jnp.int32, (tile, 1), 0) + t * tile < count
        masked = ups[part, :] * live.astype(F32).astype(BF16)
        ups[part, :] = masked
        back = nt(masked, up[...])
        logits = both[part, ranks:].T[:experts, :]
        shifted = logits - jnp.max(logits, axis=0, keepdims=True)
        powers = jnp.exp(shifted)
        total = jnp.sum(powers, axis=0, keepdims=True)
        prob = powers / total
        logp = shifted - jnp.log(total)
        ent = -jnp.sum(prob * logp, axis=0, keepdims=True)
        alive = (lax.broadcasted_iota(jnp.int32, (1, tile), 1) + t * tile < count).astype(F32)
        share = alive * prob
        share_ref[:, part] = share
        big, rest = split(prob)
        mid, small = split(rest)
        parts = jnp.concatenate([big, mid, small], axis=0).T.astype(BF16)
        spread = nn(parts, spread_by)
        low = both[part, :ranks].astype(BF16).astype(F32)
        weighted = (low * spread).astype(BF16)
        weighted_ref[part, :] = weighted
        weighted_t[:, part] = weighted.astype(F32).T.astype(BF16)
        low_grad = (2.0 * spread * back).astype(BF16)
        lowgrad_ref[part, :] = low_grad
        left_t[:ranks, part] = low_grad.astype(F32).T.astype(BF16)
        big, small = split(low * back)
        task = 2.0 * nt(group, jnp.concatenate([big, small], axis=1).astype(BF16))
        inner = jnp.sum(prob * task, axis=0, keepdims=True)
        plain = prob * (task - inner) + 50.0 * share * (logp + ent)
        plain_ref[:, part] = plain
        for kind in range(kinds):
            value = plain if kind == 0 else share * pltpu.roll(prob, experts - kind, 0)
            big, small = split(value)
            at = pl.ds(ranks + 2 * kind * experts, 2 * experts)
            left_t[at, part] = jnp.concatenate([big, small], axis=0).astype(BF16)
        return jnp.sum(share, axis=1, keepdims=True), jnp.sum(alive * ent, axis=1, keepdims=True)

    load = jnp.zeros((experts, 1), F32)
    entropy = jnp.zeros((1, 1), F32)
    for t in range(TILES + 1):
        if t < TILES:
            tok_copy(t).wait()
        if t > 0:
            ups_copy(t - 1).wait()
        if t == TILES - 1:
            frozen_copy.start()
        if t < TILES:
            part = pl.ds(t * tile, tile)
            both[part, :] = nn(tok[part, :], wide_ref[...])
        if t > 0:
            more = finish(t - 1)
            load, entropy = load + more[0], entropy + more[1]
    grad_up[...] = 2.0 * nn(weighted_t[...], ups[...])
    half = experts // 2
    lane = lax.broadcasted_iota(jnp.int32, (half, LANES), 1)
    pair_load = jnp.where(lane < LANES // 4, load[:half], load[half:])
    rest = jnp.where(lane < LANES // 4 * 3, entropy, count.astype(F32))
    stats[...] = jnp.where(lane < LANES // 2, pair_load, rest)
    used = ranks + 2 * kinds * experts
    pairs = width // (2 * LANES)
    depth = pairs.bit_length() - 1
    gate_rows = kinds * experts
    up_rows = ranks * up.shape[1] // (2 * pairs * LANES)
    per = ranks // up_rows
    for pair in range(pairs):
        kept_a, sent_a = spots(mine, pair, side, orders_a, depth)
        kept_b, sent_b = spots(mine, pair, side, orders_b, depth)
        piece = nn(left_t[:used, :], tok[:, pl.ds(pair * 2 * LANES, 2 * LANES)])
        one, two = piece[:, :LANES], piece[:, LANES:]
        gates = []
        for kind in range(kinds):
            at = ranks + 2 * kind * experts
            gates.append(piece[at : at + experts] + piece[at + experts : at + 2 * experts])
        gates = jnp.concatenate(gates, axis=0)
        keep_a[kept_a] = jnp.where(side == 0, one[:ranks], two[:ranks])
        send_a[sent_a] = jnp.where(side == 0, two[:ranks], one[:ranks])
        to = pl.ds(0, gate_rows)
        keep_b[kept_b, to] = jnp.where(side == 0, gates[:, :LANES], gates[:, LANES:])
        send_b[sent_b, to] = jnp.where(side == 0, gates[:, LANES:], gates[:, :LANES])
        keep_b[kept_b, pl.ds(gate_rows - half, half)] = stats[...]
        send_b[sent_b, pl.ds(gate_rows - half, half)] = stats[...]
        first, second = 2 * pair, 2 * pair + 1
        one = grad_up[pl.ds((first % per) * up_rows, up_rows), pl.ds(first // per * LANES, LANES)]
        two = grad_up[pl.ds((second % per) * up_rows, up_rows), pl.ds(second // per * LANES, LANES)]
        to = pl.ds(gate_rows, up_rows)
        keep_b[kept_b, to] = jnp.where(side == 0, one, two)
        send_b[sent_b, to] = jnp.where(side == 0, two, one)
    frozen_copy.wait()


def in_vmem(*arrays):
    return [pltpu.with_memory_space_constraint(array, VMEM) for array in arrays]


def in_hbm(*arrays):
    return [pltpu.with_memory_space_constraint(array, HBM) for array in arrays]


def local_grads(where, ids, gate_t, down, up, tokens, upstream, frozen, orders_a, orders_b):
    rows, width = tokens.shape
    outs = upstream.shape[1]
    experts, ranks = gate_t.shape[0], down.shape[1]
    pairs = width // (2 * LANES)
    kinds = experts // 2 + 1
    rows_b = kinds * experts + ranks * outs // (2 * pairs * LANES)
    return pl.pallas_call(
        functools.partial(local_kernel, orders_a, orders_b),
        out_shape=[
            VMEM((pairs, ranks, LANES), F32),
            VMEM((pairs, ranks, LANES), F32),
            VMEM((pairs, rows_b, LANES), F32),
            VMEM((pairs, rows_b, LANES), F32),
            VMEM((rows, ranks), BF16),
            VMEM((rows, ranks), BF16),
            VMEM((experts, rows), F32),
            VMEM((experts, rows), F32),
            VMEM((width, 2 * ranks), BF16),
            VMEM((rows, outs), BF16),
            VMEM((rows, width), BF16),
            VMEM((ranks, outs), BF16),
            VMEM((width, outs), BF16),
        ],
        in_specs=[pl.BlockSpec(memory_space=SMEM)] + [pl.BlockSpec(memory_space=HBM)] * 7,
        out_specs=[pl.BlockSpec(memory_space=VMEM)] * 13,
        scratch_shapes=[
            VMEM(ids.shape, jnp.int32),
            VMEM((experts, width), BF16),
            VMEM((width, ranks), BF16),
            VMEM((rows, 2 * ranks), F32),
            VMEM((2 * ranks, rows), BF16),
            VMEM((ranks, rows), BF16),
            VMEM((ranks, outs), F32),
            VMEM((experts // 2, LANES), F32),
            pltpu.SemaphoreType.DMA((5,)),
            pltpu.SemaphoreType.DMA((TILES,)),
            pltpu.SemaphoreType.DMA((TILES,)),
        ],
        compiler_params=pltpu.CompilerParams(vmem_limit_bytes=20 * MIB),
        cost_estimate=pl.CostEstimate(
            flops=2 * rows * width * 512, bytes_accessed=2 * rows * (width + outs), transcendentals=0
        ),
        name="local_grads",
    )(where, *in_hbm(ids, gate_t, down, up, tokens, upstream, frozen))


def project_kernel(begin, tok, weighted_ref, frozen, up_ref, *rest):
    out_ref, out, out_sem = rest[-3:]
    parts, _, cols = out.shape

    def out_copy(c):
        target = out_ref.at[:, pl.ds((begin + c) * cols, cols)]
        return pltpu.make_async_copy(out.at[c], target, out_sem.at[c])

    for c in range(parts):
        lanes = pl.ds((begin + c) * cols, cols)
        base = nn(tok[...], frozen[:, lanes])
        out[c] = (base + 2.0 * nn(weighted_ref[...], up_ref[:, lanes])).astype(BF16)
        out_copy(c).start()
    for c in range(parts):
        out_copy(c).wait()


def project(tokens, weighted, frozen, up, begin, parts, past):
    rows, width = tokens.shape
    outs, ranks = frozen.shape[1], up.shape[0]
    cols = outs // TILES
    hbm = pl.BlockSpec(memory_space=HBM)
    vmem = pl.BlockSpec(memory_space=VMEM)
    return pl.pallas_call(
        functools.partial(project_kernel, begin),
        out_shape=HBM((rows, outs), BF16),
        in_specs=[vmem] * 4 + [hbm] * len(past),
        out_specs=hbm,
        input_output_aliases={4: 0} if past else {},
        scratch_shapes=[
            VMEM((parts, rows, cols), BF16),
            pltpu.SemaphoreType.DMA((parts,)),
        ],
        compiler_params=pltpu.CompilerParams(vmem_limit_bytes=8 * MIB),
        cost_estimate=pl.CostEstimate(
            flops=2 * rows * cols * parts * (width + ranks),
            bytes_accessed=2 * (rows * width + width * cols * parts + rows * cols * parts),
            transcendentals=0,
        ),
        name="project",
    )(*in_vmem(tokens, weighted, frozen, up), *in_hbm(*past))


def owner_kernel(experts, keep_a, keep_b, recv, own_ref, stats_ref):
    count, ranks = keep_a.shape[:2]
    half = experts // 2
    at = (half + 1) * experts
    lane = lax.broadcasted_iota(jnp.int32, (experts, LANES), 1)
    shape = (half, LANES)
    for spot in range(count):
        own_ref[spot, :ranks] = keep_a[spot] + recv[spot, :ranks]
        block = keep_b[spot] + recv[spot, ranks:]
        stats = block[at - half : at]
        first = jnp.broadcast_to(stats[:, :1], shape)
        second = jnp.broadcast_to(stats[:, LANES // 4 : LANES // 4 + 1], shape)
        mine = jnp.concatenate([first, second], axis=0)
        if spot == 0:
            stats_ref[...] = jnp.where(lane < LANES // 2, mine, stats[:1])
        total = jnp.zeros((experts, LANES), F32)
        for step in range(1, half):
            both = block[step * experts : (step + 1) * experts]
            total = total + both * (mine - pltpu.roll(mine, experts - step, 0))
            total = total + pltpu.roll(both, step, 0) * (mine - pltpu.roll(mine, step, 0))
        both = block[at - experts : at - half]
        both = jnp.concatenate([both, both], axis=0)
        total = total + both * (mine - pltpu.roll(mine, half, 0))
        scale = 2.0 * experts * 100.0 / stats[:1, LANES - 1 :]
        own_ref[spot, ranks : ranks + experts] = block[:experts] + scale * total
        own_ref[spot, ranks + experts :] = block[at:]


def owner_rows(keep_a, keep_b, recv, experts):
    rows = recv.shape[1] - experts // 2 * experts
    return pl.pallas_call(
        functools.partial(owner_kernel, experts),
        out_shape=[
            jax.ShapeDtypeStruct((keep_a.shape[0], rows, LANES), F32),
            jax.ShapeDtypeStruct((experts, LANES), F32),
        ],
        compiler_params=pltpu.CompilerParams(vmem_limit_bytes=2 * MIB),
        name="owner_rows",
    )(keep_a, keep_b, recv)


def input_kernel(experts, begin, first, *refs):
    if first:
        masked, lowgrad_ref, plain_ref, share_ref, stats_ref, frozen, wide_ref = refs[:7]
        out_ref, left = refs[7:9]
    else:
        masked, left, frozen, wide_ref = refs[:4]
        out_ref = refs[5]
    out, out_sem = refs[-2:]
    parts, _, cols = out.shape

    def out_copy(c):
        target = out_ref.at[:, pl.ds((begin + c) * cols, cols)]
        return pltpu.make_async_copy(out.at[c], target, out_sem.at[c])

    if first:
        rows, ranks = lowgrad_ref.shape
        weight = stats_ref[:, :1]
        scale = 2.0 * experts * 100.0 / stats_ref[:, LANES - 1 :]
        share = share_ref[...]
        inner = jnp.sum(share * weight, axis=0, keepdims=True)
        value = plain_ref[...] + scale * share * (weight - inner)
        big, small = split(value)
        filler = jnp.zeros((ranks - 2 * experts, rows), F32)
        left[:, :ranks] = lowgrad_ref[...]
        left[:, ranks:] = jnp.concatenate([big, small, filler], axis=0).T.astype(BF16)
    for c in range(parts):
        part = pl.ds((begin + c) * cols, cols)
        out[c] = (nt(masked[...], frozen[part, :]) + nt(left[...], wide_ref[part, :])).astype(BF16)
        out_copy(c).start()
    for c in range(parts):
        out_copy(c).wait()


def input_grads(masked, lefts, frozen, wide, experts, begin, parts, past):
    rows, outs = masked.shape
    width, ranks = frozen.shape[0], wide.shape[1] // 2
    cols = 4 * LANES
    first = not past
    hbm = pl.BlockSpec(memory_space=HBM)
    vmem = pl.BlockSpec(memory_space=VMEM)
    out = HBM((rows, width), BF16)
    return pl.pallas_call(
        functools.partial(input_kernel, experts, begin, first),
        out_shape=[out, VMEM((rows, 2 * ranks), BF16)] if first else out,
        in_specs=[vmem] * (3 + len(lefts)) + [hbm] * len(past),
        out_specs=[hbm, vmem] if first else hbm,
        input_output_aliases={} if first else {4: 0},
        scratch_shapes=[
            VMEM((parts, rows, cols), BF16),
            pltpu.SemaphoreType.DMA((parts,)),
        ],
        compiler_params=pltpu.CompilerParams(vmem_limit_bytes=14 * MIB),
        cost_estimate=pl.CostEstimate(
            flops=2 * rows * cols * parts * (outs + 2 * ranks),
            bytes_accessed=2 * (rows + outs) * cols * parts + 2 * rows * outs,
            transcendentals=0,
        ),
        name="input_grads",
    )(*in_vmem(masked, *lefts, frozen, wide), *in_hbm(*past))


def clip_kernel(orders, experts, limit, where_ref, *refs):
    near, far = refs[:2], refs[2:5]
    stat_own, stat_other = refs[5:7]
    down_hbm, up_hbm, gate_hbm, load_ref, entropy_ref = refs[7:12]
    down, up, gate, squares, down_sem, sem = refs[12:]
    mine, side = where_ref[0], where_ref[1]
    half = near[0].shape[0]
    near = [(ref, spot) for ref in near for spot in range(ref.shape[0])]
    far = [(ref, spot) for ref in far for spot in range(ref.shape[0])]
    depth = (2 * half).bit_length() - 1
    ranks = down.shape[1]
    up_rows = near[0][0].shape[1] - ranks - experts
    per = ranks // up_rows
    blocks = []
    for spot in range(2 * half):
        words = []
        for order in orders:
            word = 0
            for step in range(depth):
                word += ((spot >> (depth - 1 - step)) & 1) << order[step]
            words.append(word)
        base = mine & (2 * half - 1)
        own = base ^ jnp.where(side == 0, words[0], words[1])
        other = base ^ jnp.where(side == 0, words[1], words[0])
        blocks.append((*near[spot], 2 * own + side))
        blocks.append((*far[spot], 2 * other + 1 - side))
    for ref, spot, at in blocks:
        block = ref[spot]
        square = block * block
        squares[at] = jnp.sum(square.reshape(block.shape[0] // 8, 8, LANES), axis=0)
    total = jnp.sum(jnp.sum(squares[...], axis=0), axis=(0, 1), keepdims=True)
    factor = jnp.minimum(1.0, limit / jnp.sqrt(total))
    copies = []
    for number, (ref, spot, at) in enumerate(blocks):
        rows = pl.ds(pl.multiple_of(at * LANES, LANES), LANES)
        down[rows, :] = (ref[spot, :ranks] * factor).T
        copies.append(pltpu.make_async_copy(down.at[rows], down_hbm.at[rows], down_sem.at[number]))
        copies[-1].start()
        gate[:, rows] = ref[spot, ranks : ranks + experts] * factor
        rows = pl.ds(pl.multiple_of(at % per * up_rows, up_rows), up_rows)
        lanes = pl.ds(pl.multiple_of(at // per * LANES, LANES), LANES)
        up[rows, lanes] = ref[spot, ranks + experts :] * factor
    copies.append(pltpu.make_async_copy(up, up_hbm, sem.at[0]))
    copies[-1].start()
    copies.append(pltpu.make_async_copy(gate, gate_hbm, sem.at[1]))
    copies[-1].start()
    stats = jnp.where(side == 0, stat_own[...], stat_other[...])
    stats = stats / stats[:, LANES - 1 :]
    for expert in range(experts):
        load_ref[expert] = jnp.sum(stats[expert : expert + 1, :1])
    entropy_ref[0] = jnp.sum(stats[:1, LANES // 2 : LANES // 2 + 1])
    for copy in copies:
        copy.wait()


def clip_write(where, near, far, stat_own, stat_other, ranks, outs, experts, orders):
    half = near[0].shape[0]
    width = 4 * half * LANES
    limit = math.sqrt(width * ranks + ranks * outs + width * experts)
    vmem = pl.BlockSpec(memory_space=VMEM)
    smem = pl.BlockSpec(memory_space=SMEM)
    hbm = pl.BlockSpec(memory_space=HBM)
    return pl.pallas_call(
        functools.partial(clip_kernel, orders, experts, limit),
        out_shape=[
            HBM((width, ranks), F32),
            HBM((ranks, outs), F32),
            HBM((experts, width), F32),
            jax.ShapeDtypeStruct((experts,), F32),
            jax.ShapeDtypeStruct((1,), F32),
        ],
        in_specs=[smem] + [vmem] * 7,
        out_specs=[hbm] * 3 + [smem] * 2,
        scratch_shapes=[
            VMEM((width, ranks), F32),
            VMEM((ranks, outs), F32),
            VMEM((experts, width), F32),
            VMEM((4 * half, 8, LANES), F32),
            pltpu.SemaphoreType.DMA((4 * half,)),
            pltpu.SemaphoreType.DMA((2,)),
        ],
        compiler_params=pltpu.CompilerParams(vmem_limit_bytes=8 * MIB),
        name="clip_write",
    )(where, *in_vmem(*near, *far, stat_own, stat_other))


def swap(array, masks):
    size = lax.axis_size("dp")
    return lax.ppermute(array, "dp", [(i, i ^ masks[i & 1]) for i in range(size)])


def halve(keep, recv):
    half = keep.shape[0] // 2
    send = keep[half:] + recv[half:]
    return keep[:half] + recv[:half], send


def on_device(token_ids, tokens, frozen, down, up, gate, upstream):
    experts = gate.shape[1]
    outs = frozen.shape[1]
    rows = tokens.shape[0]
    size = lax.axis_size("dp")
    bits = size.bit_length() - 2
    depth = (tokens.shape[1] // (2 * LANES)).bit_length() - 1
    rest = tuple(range(2, bits))
    orders_a = ((0, 1) + rest, (1, 0) + rest)
    orders_b = ((2, 0, 1) + rest[1:], (2, 1, 0) + rest[1:])
    me = lax.axis_index("dp")
    where = jnp.stack([me >> 1, me & 1]).astype(jnp.int32)
    ids = token_ids.reshape(rows // LANES, LANES)
    orders_g = orders_a
    masks_g = [(2 << orders_g[0][s], 2 << orders_g[1][s]) for s in range(bits)]
    masks_a = [(2 << orders_a[0][s], 2 << orders_a[1][s]) for s in range(bits)]
    masks_b = [(2 << orders_b[0][s], 2 << orders_b[1][s]) for s in range(bits)]

    keep_a, send_a, keep_b, send_b, weighted, low_grad, plain, share, wide, masked, tok, up_v, near = (
        local_grads(where, ids, gate.T, down, up, tokens, upstream, frozen, orders_a, orders_b)
    )
    split_at = keep_a.shape[1]
    filled = ()
    begin = 0
    for step in range(-1, bits):
        if step >= depth - 1:
            keep_b = send_b = keep_b + recv_b
            keep_a = send_a = keep_a + recv_a
            if step == depth - 1:
                send_b = jnp.concatenate([send_b[1:], send_b[:1]], axis=0)
                send_a = jnp.concatenate([send_a[1:], send_a[:1]], axis=0)
        elif step >= 0:
            keep_b, send_b = halve(keep_b, recv_b)
            keep_a, send_a = halve(keep_a, recv_a)
        parts = AHEAD[step + 1] if step + 1 < len(AHEAD) else 0
        if parts:
            weighted, send_a, send_b, filled = lax.optimization_barrier(
                (weighted, send_a, send_b, filled)
            )
            filled = (project(tok, weighted, near, up_v, begin, parts, filled),)
            begin += parts
        mask_a, mask_b = ((1, 1), (1, 1)) if step < 0 else (masks_a[step], masks_b[step])
        if step >= 0 and mask_a == mask_b:
            recv = swap(jnp.concatenate([send_a, send_b], axis=1), mask_a)
            recv_a, recv_b = recv[:, :split_at], recv[:, split_at:]
        else:
            recv_b = swap(send_b, mask_b)
            recv_a = swap(send_a, mask_a)
        if parts:
            recv_a, recv_b, filled = lax.optimization_barrier((recv_a, recv_b, filled))
    projected = filled[0]
    own, stats = owner_rows(keep_a, keep_b, recv, experts)
    lefts = (low_grad, plain, share, stats)
    filled = ()
    begin = 0
    tiles = tokens.shape[1] // (4 * LANES)
    turns = tuple(reversed(range(depth - 1)))
    for turn, step in enumerate(turns):
        lefts, own, filled = lax.optimization_barrier((lefts, own, filled))
        last = turn == len(turns) - 1
        parts = tiles - begin if last else CHUNKS[turn]
        if parts:
            made = input_grads(masked, lefts, near, wide, experts, begin, parts, filled)
            begin += parts
            if isinstance(made, (list, tuple)):
                filled, lefts = (made[0],), (made[1],)
            else:
                filled = (made,)
        if turn == len(turns) - 2:
            far = (swap(own, (1, 1)),)
            recv = swap(own, masks_g[step])
        else:
            recv = swap(own, masks_g[step])
        if last:
            far += (swap(own[own.shape[0] // 2 :], (1, 1)),)
            stat_other = swap(stats, (1, 1))
        recv, filled = lax.optimization_barrier((recv, filled))
        if not last:
            own = jnp.concatenate([own, recv], axis=0)
    input_grad = filled[0]
    far += (swap(recv, (1, 1)),)
    clipped_down, clipped_up, clipped_gate, load, entropy = clip_write(
        where, (own, recv), far, stats, stat_other, split_at, outs, experts, orders_g
    )
    return (
        projected,
        input_grad,
        clipped_down,
        clipped_up,
        clipped_gate.T,
        load,
        entropy.reshape(()),
    )


def solution(mesh):
    placed = (P("dp"), P("dp", None), P(), P(), P(), P(), P("dp", None))
    return jax.shard_map(
        on_device,
        mesh=mesh,
        in_specs=placed,
        out_specs=(P("dp", None), P("dp", None), P(), P(), P(), P(), P()),
        check_vma=False,
    )
```
